128 devices in a mesh: section: 4 (over x), dom: 32 (over z, y, core).
Axes of the slice: x: 4, y: 4, z: 4, core: 2. Of those that a mesh axis runs over, the one named last changes fastest.
Arguments:
- measures: bfloat16 [524288, 128], P(('section', 'dom')), may hold values from -6 to 6
- pred_columns: int32 [2, 524288], P(None, ('section', 'dom')), may hold values from 0 to 99
- bounds: int32 [2, 2], replicated, may hold values from 0 to 100
- lengths: int32 [4096], P(('section', 'dom')), may hold values from 120 to 128
- destination: int32 [524288, 1], P(('section', 'dom')), may hold values from 0 to 127; in each aligned block of 4096 rows (0 to 4095, 4096 to 8191, ...) at most 64 rows name the same one
- key_offset: int32 [524288], P(('section', 'dom')), may hold values from 0 to 2047
- group_ids: int32 [524288], P(('section', 'dom')), may hold values from 0 to 4095
- build_table: bfloat16 [262144, 128], P(('section', 'dom')), may hold values from -6 to 6
Outputs:
- group_sums: float32 [4096, 128], P(('section', 'dom'))
- top_scores: float32 [16], replicated
The draws below stay inside these ranges and needn't reach their ends.
Inputs may be any that keep to these rules, and one draw needn't show every extreme that they name: Among the rows of one device, no destination is named more than 64 times, a bound that some block reaches.
All inputs are finite; a program needn't handle non-finite values.
Results may differ from the reference program's by a relative error of at most 0.0048.
Values may be sent and summed in bfloat16 or wider, within the bound.
No kernel may reach another device: no remote copies, remote signals or barrier semaphores. Data moves between devices by JAX's collectives and lax.ppermute only.
A program may use at most 64 MiB of HBM per device.

```python
import math
import jax
import jax.numpy as jnp
import numpy as np
from jax import lax

F = 128
BLOCK = 128
NPRED = 2
TOPK = 16
ROWS_DEV = 4096
BUILD_DEV = 2048
TOTAL_ROWS = 524288
KEYS = 262144
GROUPS = 4096
CAP = 64
DEVICES = 128


def draw_bounds(key, part):
    lower_key = jax.random.fold_in(key, 11)
    upper_key = jax.random.fold_in(key, 23)
    lower = jax.random.randint(lower_key, (NPRED,), 0, 3, dtype=jnp.int32)
    upper = jax.random.randint(upper_key, (NPRED,), 98, 101, dtype=jnp.int32)
    return jnp.stack([lower, upper], axis=1)


def with_ends(array, rng, low, top_value):
    index_at = [jax.random.randint(jax.random.fold_in(rng, axis), (), 0, length) for axis, length in enumerate(array.shape)]
    longest = array.shape.index(max(array.shape))
    beside = index_at[:longest] + [(index_at[longest] + 1) % array.shape[longest]] + index_at[longest + 1:]
    return array.at[tuple(index_at)].set(low).at[tuple(beside)].set(top_value)


def block_scale(rng, shape, pieces, smallest, high):
    factor_of, own = 1.0, jax.random.fold_in(rng, 6)
    for dim, parts in pieces:
        steps = jnp.exp(jax.random.uniform(jax.random.fold_in(own, dim), (parts,), jnp.float32, smallest / len(pieces), high / len(pieces)))
        factor_of = factor_of * jnp.repeat(steps, shape[dim] // parts).reshape([-1 if axis == dim else 1 for axis in range(len(shape))])
    return factor_of


def assign_block(key, own, number, rows, number_of, top, bound, lean):
    order = jax.random.permutation(key, number_of)
    heavy_load, ordinary = load_shares(number_of, rows * top, bound, lean, True), load_shares(number_of, rows * top, bound, lean, False)
    places = jnp.arange(number_of)

    def named(sizes, offset_by):
        used = int((sizes > 0).sum())
        fixed = max(1, used // 4)
        shifted = fixed + (places - fixed + offset_by * (used - fixed)) % max(1, number_of - fixed)
        return jnp.zeros((number_of,), jnp.int32).at[order[jnp.where(places < fixed, places, shifted)]].set(jnp.asarray(sizes, jnp.int32))

    sizes = jnp.where(number % 4 == 0, named(heavy_load, number // 4), named(ordinary, number - number // 4 - 1))
    mixed = jax.random.permutation(jax.random.fold_in(own, 3), number_of)
    source_of, receiver = mixed[0:number_of // 2 * 2:2], mixed[1:number_of // 2 * 2:2]
    slack = jnp.minimum(sizes[source_of] - 1, bound - sizes[receiver]) // 2
    slack = jnp.where((source_of == order[0]) | (receiver == order[0]) | (sizes[receiver] == 0), 0, jnp.maximum(slack, 0))
    shifted = jax.random.randint(jax.random.fold_in(own, 4), (number_of // 2,), 0, 1 << 20) % (slack + 1)
    sizes = sizes.at[source_of].add(-shifted).at[receiver].add(shifted)
    labels = jnp.searchsorted(jnp.cumsum(sizes), jnp.arange(rows * top), side="right").astype(jnp.int32)
    listing = labels.reshape(top, rows).T
    listing = listing[jax.random.permutation(jax.random.fold_in(own, 1), rows)]
    offset_by = jax.random.randint(jax.random.fold_in(own, 2), (rows, 1), 0, top)
    return jnp.take_along_axis(listing, (jnp.arange(top)[None, :] + offset_by) % top, axis=1)


def load_shares(count, total, limit, skew, full):
    loads = [(1 << 20) // math.isqrt(grade ** skew) + 1 for grade in range(1, count + 1)]
    largest = limit if full else min(limit, max(-(-total // count), total * loads[0] // sum(loads)))
    least = 1 if total - largest >= count - 1 else 0
    given, rest = [largest] + [least] * (count - 1), total - largest - least * (count - 1)
    while rest > 0:
        free = [i for i in range(1, count) if given[i] < largest] or [i for i in range(1, count) if given[i] < limit]
        mass, left = sum([loads[i] for i in free]), rest
        for i in free:
            addition = min(limit - given[i], max(1, left * loads[i] // mass), rest)
            given[i] = given[i] + addition
            rest = rest - addition
    return np.array(given)


def bell_draw(key, shape, width, limit, split=(), kind=jnp.bfloat16):
    gain = block_scale(key, shape, split, -0.22, 0.18) if split else 1.0
    values = jax.random.normal(key, shape, jnp.float32) * width * gain
    return jnp.minimum(jnp.maximum(values, -limit), limit).astype(kind)


def setup_inputs(seed: int = 0) -> dict:
    key_list = jax.random.split(jax.random.key(seed), 9)
    measures = bell_draw(key_list[0], (TOTAL_ROWS, F), 1.0, 6.0, ((0, 128),))
    pred_columns = with_ends(jax.random.randint(key_list[1], (NPRED, TOTAL_ROWS), 0, 100), jax.random.fold_in(key_list[1], 1), 0, 99).astype(jnp.int32)
    bounds = draw_bounds(jax.random.fold_in(key_list[8], 71), 0)
    lengths = with_ends(jax.random.randint(key_list[3], (TOTAL_ROWS // BLOCK,), BLOCK - 8, BLOCK + 1), jax.random.fold_in(key_list[3], 1), BLOCK - 8, BLOCK).astype(jnp.int32)
    destination_keys = jax.random.split(jax.random.fold_in(key_list[4], 1), TOTAL_ROWS // ROWS_DEV)
    destination_turns = jax.random.permutation(jax.random.fold_in(key_list[4], 3), TOTAL_ROWS // ROWS_DEV)
    destination = jax.vmap(lambda own, number: assign_block(jax.random.fold_in(key_list[4], 2), own, number, ROWS_DEV, DEVICES, 1, CAP, 2))(destination_keys, destination_turns).reshape((TOTAL_ROWS, 1))
    key_offset = with_ends(jax.random.randint(key_list[5], (TOTAL_ROWS,), 0, BUILD_DEV), jax.random.fold_in(key_list[5], 1), 0, BUILD_DEV - 1).astype(jnp.int32)
    group_ids = with_ends(jax.random.randint(key_list[6], (TOTAL_ROWS,), 0, GROUPS), jax.random.fold_in(key_list[6], 1), 0, GROUPS - 1).astype(jnp.int32)
    build_table = bell_draw(key_list[7], (KEYS, F), 1.0, 6.0, ((0, 128),))
    return dict(measures=measures, pred_columns=pred_columns, bounds=bounds, lengths=lengths, destination=destination, key_offset=key_offset, group_ids=group_ids, build_table=build_table)


def reference(measures, pred_columns, bounds, lengths, destination, key_offset, group_ids, build_table):
    total_rows = measures.shape[0]
    within = (lengths[:, None] > jnp.arange(BLOCK, dtype=jnp.int32)[None, :]).reshape(total_rows)
    passes = jnp.all((pred_columns >= bounds[:, 0:1]) & (pred_columns < bounds[:, 1:2]), axis=0)
    usable = within & passes
    join_keys = (destination[:, 0] * BUILD_DEV + key_offset).astype(jnp.int32)
    attributes = jnp.take(build_table, join_keys, axis=0)
    joined = measures.astype(jnp.float32) * attributes.astype(jnp.float32)
    joined = jnp.where(usable[:, None], joined, jnp.zeros_like(joined)).astype(jnp.bfloat16)
    group_sums = jax.ops.segment_sum(joined.astype(jnp.float32), group_ids, num_segments=GROUPS)
    scores = jnp.mean(group_sums, axis=1)
    top_scores = lax.top_k(scores, TOPK)[0]
    return group_sums, top_scores
```

```python
import jax
import jax.numpy as jnp
from jax import lax
from jax.experimental import pallas as pl
from jax.experimental.pallas import tpu as pltpu
from jax.sharding import Mesh
from jax.sharding import PartitionSpec as P

BLOCK = 128
TOPK = 16
SLOTS = 64
AREA = 72
DESTS = 128
BF = jnp.bfloat16
F32 = jnp.float32
I32 = jnp.int32
NT = (((1,), (1,)), ((), ()))
VMEM = pl.BlockSpec(memory_space=pltpu.VMEM)
SMEM = pl.BlockSpec(memory_space=pltpu.SMEM)


def pack_kernel(
    me_ref, bounds_ref, lengths_ref, measures_ref, preds_ref, dest_ref, keys_ref, groups_ref,
    own_ref, other_ref, area_ref, place_ref, place_smem, sem,
):
    rows = measures_ref.shape[0]
    wide = 2 * BLOCK
    half = DESTS // 2
    me = me_ref[0]
    lane = lax.broadcasted_iota(I32, (1, BLOCK), 1)
    before = (
        lax.broadcasted_iota(I32, (wide, wide), 0) < lax.broadcasted_iota(I32, (wide, wide), 1)
    ).astype(F32).astype(BF)
    count_of = jnp.concatenate([before, jnp.ones((wide, wide), BF)], axis=1)
    dest_ids = lax.broadcasted_iota(I32, (DESTS, wide), 0)
    slot_ids = lax.broadcasted_iota(I32, (SLOTS, wide), 0)
    carry = jnp.zeros((DESTS, wide), F32)
    packed = jnp.zeros((DESTS, 4 * SLOTS), F32)
    for step in range(rows // wide):
        parts = []
        for b in (2 * step, 2 * step + 1):
            at = pl.ds(b * BLOCK, BLOCK)
            ok = lane < lengths_ref[b]
            for c in range(preds_ref.shape[0]):
                v = preds_ref[c : c + 1, at]
                ok = ok & (v >= bounds_ref[c, 0]) & (v < bounds_ref[c, 1])
            d = dest_ref[b : b + 1, :]
            spot = ((d & 1) ^ me) * half + (d >> 1)
            parts.append(jnp.where(ok, spot, -1))
        target = jnp.concatenate(parts, axis=1)
        keys = jnp.concatenate([keys_ref[2 * step : 2 * step + 1, :], keys_ref[2 * step + 1 : 2 * step + 2, :]], axis=1)
        groups = jnp.concatenate([groups_ref[2 * step : 2 * step + 1, :], groups_ref[2 * step + 1 : 2 * step + 2, :]], axis=1)
        hit = dest_ids == target
        names = hit.astype(F32)
        names16 = names.astype(BF)
        counts = jnp.dot(names16, count_of, preferred_element_type=F32)
        slot = jnp.sum(names * (counts[:, :wide] + carry), axis=0, keepdims=True).astype(I32)
        carry = carry + counts[:, wide:]
        place = jnp.where(target >= 0, target * AREA + slot, DESTS * AREA)
        place_ref[2 * step : 2 * step + 1, :] = place[:, :BLOCK]
        place_ref[2 * step + 1 : 2 * step + 2, :] = place[:, BLOCK:]
        mine = slot_ids == slot
        values = [
            jnp.where(mine, part.astype(F32), 0.0).astype(BF)
            for part in (keys >> 8, keys & 255, groups >> 8, groups & 255)
        ]
        packed = packed + lax.dot_general(
            names16, jnp.concatenate(values, axis=0), NT, preferred_element_type=F32
        )
    copy = pltpu.make_async_copy(place_ref, place_smem, sem)
    copy.start()

    def clear(i, _):
        area_ref[pl.ds(pl.multiple_of(i * AREA, 8), AREA), :] = jnp.zeros((AREA, BLOCK), F32)
        return 0

    lax.fori_loop(0, DESTS, clear, 0, unroll=4)
    for d in range(DESTS):
        area_ref[d * AREA + SLOTS : d * AREA + SLOTS + 1, :] = packed[d : d + 1, :BLOCK]
        area_ref[d * AREA + SLOTS + 1 : d * AREA + SLOTS + 2, :] = packed[d : d + 1, BLOCK:]
    copy.wait()

    def put(i, _):
        x = measures_ref[pl.ds(pl.multiple_of(i * 16, 16), 16), :].astype(F32)
        for u in range(16):
            p = place_smem[i // 8, (i % 8) * 16 + u]
            area_ref[pl.ds(p, 1), :] = x[u : u + 1, :]
        return 0

    lax.fori_loop(0, rows // 16, put, 0, unroll=2)

    def give(i, _):
        at = pl.ds(pl.multiple_of(i * AREA, 8), AREA)
        own_ref[i] = area_ref[at, :].astype(BF)
        later = pl.ds(pl.multiple_of((i + half) * AREA, 8), AREA)
        other_ref[i] = area_ref[later, :].astype(BF)
        return 0

    lax.fori_loop(0, half, give, 0, unroll=2)


def pack(me, bounds, lengths, measures, preds, dest, keys, groups):
    half = DESTS // 2
    out = jax.ShapeDtypeStruct((half, AREA, BLOCK), BF)
    rows = measures.shape[0]
    return pl.pallas_call(
        pack_kernel,
        out_shape=(out, out),
        in_specs=[SMEM, SMEM, SMEM, VMEM, VMEM, VMEM, VMEM, VMEM],
        out_specs=(VMEM, VMEM),
        scratch_shapes=[
            pltpu.VMEM((DESTS * AREA + 8, BLOCK), F32),
            pltpu.VMEM((rows // BLOCK, BLOCK), I32),
            pltpu.SMEM((rows // BLOCK, BLOCK), I32),
            pltpu.SemaphoreType.DMA,
        ],
        compiler_params=pltpu.CompilerParams(vmem_limit_bytes=32 << 20),
        name="pack",
    )(me, bounds, lengths, measures, preds, dest, keys, groups)


def join_kernel(me_ref, got_ref, table_ref, own_ref, other_ref, pair_ref, sums_ref, keyt_ref, group_ref):
    chips = got_ref.shape[0]
    first = got_ref[:, SLOTS : SLOTS + 8, :].astype(F32)
    second = got_ref[:, AREA + SLOTS : AREA + SLOTS + 8, :].astype(F32)
    ka, kb = first[:, 0, :], second[:, 0, :]
    ga, gb = first[:, 1, :], second[:, 1, :]

    def halves(a, b):
        return (
            jnp.concatenate([a[:, :SLOTS], b[:, :SLOTS]], axis=1),
            jnp.concatenate([a[:, SLOTS:], b[:, SLOTS:]], axis=1),
        )

    key_hi, key_lo = halves(ka, kb)
    grp_hi, grp_lo = halves(ga, gb)
    square = jnp.zeros((BLOCK - chips, BLOCK), F32)
    keyt_ref[...] = jnp.concatenate([key_hi * 256.0 + key_lo, grp_hi], axis=0).T
    group_ref[0] = grp_hi
    group_ref[1] = grp_lo
    tab = jnp.concatenate([table_ref[:1024, :], table_ref[1024:, :]], axis=1)
    ids = lax.broadcasted_iota(I32, (BLOCK, 256), 1).astype(F32).astype(BF)
    one = jnp.ones((), BF)
    zero = jnp.zeros((), BF)
    for p in range(chips):
        key = jnp.broadcast_to(keyt_ref[:, p : p + 1], (BLOCK, BLOCK))
        top = jnp.broadcast_to(keyt_ref[:, chips + p : chips + p + 1], (BLOCK, BLOCK))
        upper = key >= 1024.0
        key = jnp.where(upper, key - 1024.0, key)
        cols = []
        for t in range(4):
            k = (key - 256.0 * t).astype(BF)
            k = jnp.concatenate([k, k], axis=1)
            cols.append(jnp.where(ids == k, one, zero))
        found = jnp.dot(jnp.concatenate(cols, axis=1), tab, preferred_element_type=F32)
        row = jnp.where(upper, found[:, BLOCK:], found[:, :BLOCK])
        pay = jnp.concatenate([got_ref[p, :SLOTS, :], got_ref[p, AREA : AREA + SLOTS, :]], axis=0)
        joined = pay.astype(F32) * row
        high = top >= 8.0
        none = jnp.zeros_like(joined)
        pair_ref[p * BLOCK : (p + 1) * BLOCK, :BLOCK] = jnp.where(high, none, joined).astype(BF)
        pair_ref[p * BLOCK : (p + 1) * BLOCK, BLOCK:] = jnp.where(high, joined, none).astype(BF)

    rows_at = lax.broadcasted_iota(I32, (256, BLOCK), 0).astype(F32).astype(BF)
    per = 8
    for k in range(chips // per):
        low3 = []
        for p in range(k * per, (k + 1) * per):
            hi = group_ref[0, p : p + 1, :]
            low3.append((jnp.where(hi >= 8.0, hi - 8.0, hi), group_ref[1, p : p + 1, :]))
        block = pair_ref[k * per * BLOCK : (k + 1) * per * BLOCK, :]
        for t in range(8):
            cols = []
            for hi, lo in low3:
                v = jnp.where(hi == float(t), lo, -1.0).astype(BF)
                cols.append(jnp.where(rows_at == jnp.broadcast_to(v, (256, BLOCK)), one, zero))
            part = jnp.dot(jnp.concatenate(cols, axis=1), block, preferred_element_type=F32)
            at = pl.ds(t * 256, 256)
            if k == 0:
                sums_ref[at, :] = part
            else:
                sums_ref[at, :] = sums_ref[at, :] + part

    me = me_ref[0]
    for i in range(64):
        col = (i // 32) * BLOCK
        base = (i % 32) * 64
        mine = pl.ds(pl.multiple_of(base + me * 32, 8), 32)
        theirs = pl.ds(pl.multiple_of(base + (1 - me) * 32, 8), 32)
        own_ref[i] = sums_ref[mine, col : col + BLOCK]
        other_ref[i] = sums_ref[theirs, col : col + BLOCK].astype(BF)


def join(me, got, table):
    chips = got.shape[0]
    return pl.pallas_call(
        join_kernel,
        out_shape=(
            jax.ShapeDtypeStruct((chips, 32, BLOCK), F32),
            jax.ShapeDtypeStruct((chips, 32, BLOCK), BF),
        ),
        in_specs=[SMEM, VMEM, VMEM],
        out_specs=(VMEM, VMEM),
        scratch_shapes=[
            pltpu.VMEM((chips * BLOCK, 2 * BLOCK), BF),
            pltpu.VMEM((2048, 2 * BLOCK), F32),
            pltpu.VMEM((BLOCK, BLOCK), F32),
            pltpu.VMEM((2, chips, BLOCK), F32),
        ],
        compiler_params=pltpu.CompilerParams(vmem_limit_bytes=40 << 20),
        name="join",
    )(me, got, table)


def merge_kernel(own_ref, got_ref, out_ref):
    chips, rows, _ = own_ref.shape
    total = (own_ref[...] + got_ref[...].astype(F32)).astype(BF)
    out_ref[:, :rows, :] = total
    ones = jnp.ones((8, BLOCK), BF)
    flat = total.reshape(chips * rows, BLOCK)
    means = lax.dot_general(ones, flat, NT, preferred_element_type=F32)
    score = jnp.concatenate(
        [means[0:1, n * BLOCK : (n + 1) * BLOCK] for n in range(chips * rows // BLOCK)], axis=0
    )
    score = (score * (1.0 / BLOCK)).astype(BF)
    out_ref[:, rows:, :] = jnp.broadcast_to(score[None], (chips, *score.shape))


def merge(own, got):
    chips, rows, _ = own.shape
    return pl.pallas_call(
        merge_kernel,
        out_shape=jax.ShapeDtypeStruct((chips, rows + chips * rows // BLOCK, BLOCK), BF),
        in_specs=[VMEM, VMEM],
        out_specs=VMEM,
        compiler_params=pltpu.CompilerParams(vmem_limit_bytes=16 << 20),
        name="merge",
    )(own, got)


def total_kernel(got_ref, sums_ref, score_ref):
    rows = sums_ref.shape[0]
    total = got_ref[0].astype(F32)
    for p in range(1, got_ref.shape[0]):
        total = total + got_ref[p].astype(F32)
    sums_ref[...] = total[:rows, :]
    score_ref[...] = total[rows:, :]


def total(got, rows):
    return pl.pallas_call(
        total_kernel,
        out_shape=(
            jax.ShapeDtypeStruct((rows, BLOCK), F32),
            jax.ShapeDtypeStruct((got.shape[1] - rows, BLOCK), F32),
        ),
        in_specs=[VMEM],
        out_specs=(VMEM, VMEM),
        compiler_params=pltpu.CompilerParams(vmem_limit_bytes=8 << 20),
        name="total",
    )(got)


def leaders_kernel(a_ref, b_ref, out_ref):
    x = jnp.concatenate([a_ref[...], b_ref[...]], axis=0)
    lane = lax.broadcasted_iota(I32, (1, BLOCK), 1)
    taken = jnp.zeros((1, 1), F32)
    out = jnp.full((1, BLOCK), -jnp.inf, F32)
    place = lane.astype(F32)
    for _ in range(TOPK):
        best = jnp.max(jnp.max(x, axis=0, keepdims=True), axis=1, keepdims=True)
        same = x == best
        count = jnp.sum(
            jnp.sum(same.astype(F32), axis=0, keepdims=True), axis=1, keepdims=True
        )
        out = jnp.where((place >= taken) & (place < taken + count), best, out)
        taken = taken + count
        x = jnp.where(same, -jnp.inf, x)
    out_ref[...] = out[:, :TOPK]


def leaders(a, b):
    return pl.pallas_call(
        leaders_kernel,
        out_shape=jax.ShapeDtypeStruct((1, TOPK), F32),
        in_specs=[VMEM, VMEM],
        out_specs=VMEM,
        compiler_params=pltpu.CompilerParams(vmem_limit_bytes=4 << 20),
        name="leaders",
    )(a, b)


CHIPS = ("section", "dom_0", "dom_1")
CORE = "dom_2"
DEVICES = (*CHIPS, CORE)
SWAP = [(0, 1), (1, 0)]


def on_device(
    measures, pred_columns, bounds, lengths, destination, key_offset, group_ids, build_table
):
    blocks = measures.shape[0] // BLOCK
    me = lax.axis_index(CORE).astype(I32).reshape(1)

    def lanes(v):
        return v.reshape(blocks, BLOCK)

    own, other = pack(
        me, bounds, lengths, measures, pred_columns, lanes(destination), lanes(key_offset), lanes(group_ids)
    )
    partner = lax.ppermute(other, CORE, SWAP)
    packets = jnp.concatenate([own, partner], axis=1)
    got = lax.all_to_all(packets, CHIPS, split_axis=0, concat_axis=0, tiled=True)
    mine, theirs = join(me, got, build_table)
    pair = merge(mine, lax.ppermute(theirs, CORE, SWAP))
    arrived = lax.all_to_all(pair, CHIPS, split_axis=0, concat_axis=0, tiled=True)
    group_sums, scores = total(arrived, 32)
    top = leaders(scores, lax.ppermute(scores, CORE, SWAP))
    return group_sums, top.reshape(TOPK)


def solution(mesh):
    finer = Mesh(mesh.devices.reshape(mesh.shape["section"], 4, 4, 2), DEVICES)
    return jax.shard_map(
        on_device,
        mesh=finer,
        in_specs=(
            P(DEVICES, None),
            P(None, DEVICES),
            P(),
            P(DEVICES),
            P(DEVICES, None),
            P(DEVICES),
            P(DEVICES),
            P(DEVICES, None),
        ),
        out_specs=(P(DEVICES, None), P()),
        check_vma=False,
    )
```

```python
import jax
import jax.numpy as jnp
from jax import lax
from jax.experimental import pallas as pl
from jax.experimental.pallas import tpu as pltpu
from jax.sharding import Mesh
from jax.sharding import PartitionSpec as P

BLOCK = 128
TOPK = 16
SLOTS = 64
AREA = 72
DESTS = 128
PIECES = 4
BF = jnp.bfloat16
F32 = jnp.float32
I32 = jnp.int32
NT = (((1,), (1,)), ((), ()))
VMEM = pl.BlockSpec(memory_space=pltpu.VMEM)
SMEM = pl.BlockSpec(memory_space=pltpu.SMEM)
HBM = pl.BlockSpec(memory_space=pltpu.HBM)


def pack_kernel(
    bounds_hbm, lengths_hbm, measures_hbm, preds_hbm, dest_hbm, keys_hbm, groups_hbm, out_hbm,
    bounds_ref, lengths_ref, measures_ref, preds_ref, dest_ref, keys_ref, groups_ref,
    area_ref, area16_ref, place_ref, place_smem, sems,
):
    rows = measures_ref.shape[0]
    wide = 2 * BLOCK
    sources = (preds_hbm, dest_hbm, keys_hbm, groups_hbm, bounds_hbm, lengths_hbm, measures_hbm)
    targets = (preds_ref, dest_ref, keys_ref, groups_ref, bounds_ref, lengths_ref, measures_ref)
    loads = [
        pltpu.make_async_copy(source, target, sems.at[n])
        for n, (source, target) in enumerate(zip(sources, targets))
    ]
    for load in loads:
        load.start()

    def clear(i, _):
        area_ref[pl.ds(pl.multiple_of(i * AREA, 8), AREA), :] = jnp.zeros((AREA, BLOCK), F32)
        return 0

    lax.fori_loop(0, DESTS, clear, 0, unroll=4)
    for load in loads[:-1]:
        load.wait()
    lane = lax.broadcasted_iota(I32, (1, BLOCK), 1)
    before = (
        lax.broadcasted_iota(I32, (wide, wide), 0) < lax.broadcasted_iota(I32, (wide, wide), 1)
    ).astype(F32).astype(BF)
    count_of = jnp.concatenate([before, jnp.ones((wide, wide), BF)], axis=1)
    dest_ids = lax.broadcasted_iota(I32, (DESTS, wide), 0)
    slot_ids = lax.broadcasted_iota(I32, (SLOTS, wide), 0)
    carry = jnp.zeros((DESTS, wide), F32)
    packed = jnp.zeros((DESTS, 4 * SLOTS), F32)

    def pair(ref, step):
        return jnp.concatenate(
            [ref[2 * step : 2 * step + 1, :], ref[2 * step + 1 : 2 * step + 2, :]], axis=1
        )

    for step in range(rows // wide):
        at = pl.ds(step * wide, wide)
        ok = jnp.concatenate([lane < lengths_ref[2 * step], lane < lengths_ref[2 * step + 1]], axis=1)
        for c in range(preds_ref.shape[0]):
            v = preds_ref[c : c + 1, at]
            ok = ok & (v >= bounds_ref[c, 0]) & (v < bounds_ref[c, 1])
        target = jnp.where(ok, pair(dest_ref, step), -1)
        keys = pair(keys_ref, step)
        groups = pair(groups_ref, step)
        names = (dest_ids == target).astype(F32)
        names16 = names.astype(BF)
        counts = jnp.dot(names16, count_of, preferred_element_type=F32)
        slot = jnp.sum(names * (counts[:, :wide] + carry), axis=0, keepdims=True).astype(I32)
        carry = carry + counts[:, wide:]
        place = jnp.where(ok, target * AREA + slot, DESTS * AREA)
        place_ref[2 * step : 2 * step + 1, :] = place[:, :BLOCK]
        place_ref[2 * step + 1 : 2 * step + 2, :] = place[:, BLOCK:]
        mine = slot_ids == slot
        values = [
            jnp.where(mine, part.astype(F32), 0.0).astype(BF)
            for part in (keys >> 8, keys & 255, groups >> 8, groups & 255)
        ]
        packed = packed + lax.dot_general(
            names16, jnp.concatenate(values, axis=0), NT, preferred_element_type=F32
        )
    copy = pltpu.make_async_copy(place_ref, place_smem, sems.at[len(loads)])
    copy.start()
    for d in range(DESTS):
        area_ref[d * AREA + SLOTS : d * AREA + SLOTS + 1, :] = packed[d : d + 1, :BLOCK]
        area_ref[d * AREA + SLOTS + 1 : d * AREA + SLOTS + 2, :] = packed[d : d + 1, BLOCK:]
    loads[-1].wait()
    copy.wait()

    def put(b, _):
        for k in range(BLOCK // 16):
            x = measures_ref[pl.ds(pl.multiple_of(b * BLOCK + k * 16, 16), 16), :].astype(F32)
            for u in range(16):
                area_ref[pl.ds(place_smem[b, k * 16 + u], 1), :] = x[u : u + 1, :]
        return 0

    lax.fori_loop(0, rows // BLOCK, put, 0)

    def give(i, _):
        area16_ref[i] = area_ref[pl.ds(pl.multiple_of(i * AREA, 8), AREA), :].astype(BF)
        return 0

    stores = []
    for n in range(PIECES):
        part = DESTS // PIECES
        lax.fori_loop(n * part, (n + 1) * part, give, 0, unroll=4)
        stores.append(
            pltpu.make_async_copy(
                area16_ref.at[pl.ds(n * part, part)], out_hbm.at[pl.ds(n * part, part)], sems.at[8 + n]
            )
        )
        stores[-1].start()
    for store in stores:
        store.wait()


def pack(bounds, lengths, measures, preds, dest, keys, groups):
    rows = measures.shape[0]
    blocks = rows // BLOCK
    return pl.pallas_call(
        pack_kernel,
        out_shape=jax.ShapeDtypeStruct((DESTS, AREA, BLOCK), BF),
        in_specs=[HBM] * 7,
        out_specs=HBM,
        scratch_shapes=[
            pltpu.SMEM(bounds.shape, I32),
            pltpu.SMEM(lengths.shape, I32),
            pltpu.VMEM(measures.shape, BF),
            pltpu.VMEM(preds.shape, I32),
            pltpu.VMEM((blocks, BLOCK), I32),
            pltpu.VMEM((blocks, BLOCK), I32),
            pltpu.VMEM((blocks, BLOCK), I32),
            pltpu.VMEM((DESTS * AREA + 8, BLOCK), F32),
            pltpu.VMEM((DESTS, AREA, BLOCK), BF),
            pltpu.VMEM((blocks, BLOCK), I32),
            pltpu.SMEM((blocks, BLOCK), I32),
            pltpu.SemaphoreType.DMA((8 + PIECES,)),
        ],
        compiler_params=pltpu.CompilerParams(vmem_limit_bytes=58 << 20),
        name="pack",
    )(bounds, lengths, measures, preds, dest, keys, groups)


def join_kernel(me_ref, got_ref, table_ref, own_ref, other_ref, pair_ref, sums_ref, keyt_ref, group_ref):
    chips = got_ref.shape[0] // 2
    first = got_ref[:chips, SLOTS : SLOTS + 8, :].astype(F32)
    second = got_ref[chips:, SLOTS : SLOTS + 8, :].astype(F32)
    ka, kb = first[:, 0, :], second[:, 0, :]
    ga, gb = first[:, 1, :], second[:, 1, :]

    def halves(a, b):
        return (
            jnp.concatenate([a[:, :SLOTS], b[:, :SLOTS]], axis=1),
            jnp.concatenate([a[:, SLOTS:], b[:, SLOTS:]], axis=1),
        )

    key_hi, key_lo = halves(ka, kb)
    grp_hi, grp_lo = halves(ga, gb)
    keyt_ref[...] = jnp.concatenate([key_hi * 256.0 + key_lo, grp_hi], axis=0).T
    group_ref[0] = grp_hi
    group_ref[1] = grp_lo
    tab = jnp.concatenate([table_ref[:1024, :], table_ref[1024:, :]], axis=1)
    ids = lax.broadcasted_iota(I32, (BLOCK, 256), 1).astype(F32).astype(BF)
    one = jnp.ones((), BF)
    zero = jnp.zeros((), BF)
    for p in range(chips):
        key = jnp.broadcast_to(keyt_ref[:, p : p + 1], (BLOCK, BLOCK))
        top = jnp.broadcast_to(keyt_ref[:, chips + p : chips + p + 1], (BLOCK, BLOCK))
        upper = key >= 1024.0
        key = jnp.where(upper, key - 1024.0, key)
        cols = []
        for t in range(4):
            k = (key - 256.0 * t).astype(BF)
            k = jnp.concatenate([k, k], axis=1)
            cols.append(jnp.where(ids == k, one, zero))
        found = jnp.dot(jnp.concatenate(cols, axis=1), tab, preferred_element_type=F32)
        row = jnp.where(upper, found[:, BLOCK:], found[:, :BLOCK])
        pay = jnp.concatenate([got_ref[p, :SLOTS, :], got_ref[chips + p, :SLOTS, :]], axis=0)
        joined = pay.astype(F32) * row
        high = top >= 8.0
        none = jnp.zeros_like(joined)
        pair_ref[p * BLOCK : (p + 1) * BLOCK, :BLOCK] = jnp.where(high, none, joined).astype(BF)
        pair_ref[p * BLOCK : (p + 1) * BLOCK, BLOCK:] = jnp.where(high, joined, none).astype(BF)

    rows_at = lax.broadcasted_iota(I32, (256, BLOCK), 0).astype(F32).astype(BF)
    per = 8
    for k in range(chips // per):
        low3 = []
        for p in range(k * per, (k + 1) * per):
            hi = group_ref[0, p : p + 1, :]
            low3.append((jnp.where(hi >= 8.0, hi - 8.0, hi), group_ref[1, p : p + 1, :]))
        block = pair_ref[k * per * BLOCK : (k + 1) * per * BLOCK, :]
        for t in range(8):
            cols = []
            for hi, lo in low3:
                v = jnp.where(hi == float(t), lo, -1.0).astype(BF)
                cols.append(jnp.where(rows_at == jnp.broadcast_to(v, (256, BLOCK)), one, zero))
            part = jnp.dot(jnp.concatenate(cols, axis=1), block, preferred_element_type=F32)
            at = pl.ds(t * 256, 256)
            if k == 0:
                sums_ref[at, :] = part
            else:
                sums_ref[at, :] = sums_ref[at, :] + part

    me = me_ref[0]
    for i in range(64):
        col = (i // 32) * BLOCK
        base = (i % 32) * 64
        mine = pl.ds(pl.multiple_of(base + me * 32, 8), 32)
        theirs = pl.ds(pl.multiple_of(base + (1 - me) * 32, 8), 32)
        own_ref[i] = sums_ref[mine, col : col + BLOCK]
        other_ref[i] = sums_ref[theirs, col : col + BLOCK].astype(BF)


def join(me, got, table):
    chips = got.shape[0] // 2
    return pl.pallas_call(
        join_kernel,
        out_shape=(
            jax.ShapeDtypeStruct((chips, 32, BLOCK), F32),
            jax.ShapeDtypeStruct((chips, 32, BLOCK), BF),
        ),
        in_specs=[SMEM, VMEM, VMEM],
        out_specs=(VMEM, VMEM),
        scratch_shapes=[
            pltpu.VMEM((chips * BLOCK, 2 * BLOCK), BF),
            pltpu.VMEM((2048, 2 * BLOCK), F32),
            pltpu.VMEM((BLOCK, BLOCK), F32),
            pltpu.VMEM((2, chips, BLOCK), F32),
        ],
        compiler_params=pltpu.CompilerParams(vmem_limit_bytes=40 << 20),
        name="join",
    )(me, got, table)


def merge_kernel(own_ref, got_ref, out_ref):
    chips, rows, _ = own_ref.shape
    total = (own_ref[...] + got_ref[...].astype(F32)).astype(BF)
    out_ref[:, :rows, :] = total
    ones = jnp.ones((8, BLOCK), BF)
    flat = total.reshape(chips * rows, BLOCK)
    means = lax.dot_general(ones, flat, NT, preferred_element_type=F32)
    score = jnp.concatenate(
        [means[0:1, n * BLOCK : (n + 1) * BLOCK] for n in range(chips * rows // BLOCK)], axis=0
    )
    score = (score * (1.0 / BLOCK)).astype(BF)
    out_ref[:, rows:, :] = jnp.broadcast_to(score[None], (chips, *score.shape))


def merge(own, got):
    chips, rows, _ = own.shape
    return pl.pallas_call(
        merge_kernel,
        out_shape=jax.ShapeDtypeStruct((chips, rows + chips * rows // BLOCK, BLOCK), BF),
        in_specs=[VMEM, VMEM],
        out_specs=VMEM,
        compiler_params=pltpu.CompilerParams(vmem_limit_bytes=16 << 20),
        name="merge",
    )(own, got)


def total_kernel(got_ref, sums_ref, score_ref):
    rows = sums_ref.shape[0]
    total = got_ref[0].astype(F32)
    for p in range(1, got_ref.shape[0]):
        total = total + got_ref[p].astype(F32)
    sums_ref[...] = total[:rows, :]
    score_ref[...] = total[rows:, :]


def total(got, rows):
    return pl.pallas_call(
        total_kernel,
        out_shape=(
            jax.ShapeDtypeStruct((rows, BLOCK), F32),
            jax.ShapeDtypeStruct((got.shape[1] - rows, BLOCK), F32),
        ),
        in_specs=[VMEM],
        out_specs=(VMEM, VMEM),
        compiler_params=pltpu.CompilerParams(vmem_limit_bytes=8 << 20),
        name="total",
    )(got)


def leaders_kernel(a_ref, b_ref, out_ref):
    x = jnp.concatenate([a_ref[...], b_ref[...]], axis=0)
    lane = lax.broadcasted_iota(I32, (1, BLOCK), 1)
    taken = jnp.zeros((1, 1), F32)
    out = jnp.full((1, BLOCK), -jnp.inf, F32)
    place = lane.astype(F32)
    for _ in range(TOPK):
        best = jnp.max(jnp.max(x, axis=0, keepdims=True), axis=1, keepdims=True)
        same = x == best
        count = jnp.sum(
            jnp.sum(same.astype(F32), axis=0, keepdims=True), axis=1, keepdims=True
        )
        out = jnp.where((place >= taken) & (place < taken + count), best, out)
        taken = taken + count
        x = jnp.where(same, -jnp.inf, x)
    out_ref[...] = out[:, :TOPK]


def leaders(a, b):
    return pl.pallas_call(
        leaders_kernel,
        out_shape=jax.ShapeDtypeStruct((1, TOPK), F32),
        in_specs=[VMEM, VMEM],
        out_specs=VMEM,
        compiler_params=pltpu.CompilerParams(vmem_limit_bytes=4 << 20),
        name="leaders",
    )(a, b)


CHIPS = ("section", "dom_0", "dom_1")
CORE = "dom_2"
DEVICES = (*CHIPS, CORE)
SWAP = [(0, 1), (1, 0)]


def on_device(
    measures, pred_columns, bounds, lengths, destination, key_offset, group_ids, build_table
):
    blocks = measures.shape[0] // BLOCK
    me = lax.axis_index(CORE).astype(I32).reshape(1)

    def lanes(v):
        return v.reshape(blocks, BLOCK)

    me, bounds = lax.optimization_barrier((me, bounds))
    packets = pack(
        bounds, lengths, measures, pred_columns, lanes(destination), lanes(key_offset), lanes(group_ids)
    )
    got = lax.all_to_all(packets, DEVICES, split_axis=0, concat_axis=0, tiled=True)
    mine, theirs = join(me, got, build_table)
    pair = merge(mine, lax.ppermute(theirs, CORE, SWAP))
    arrived = lax.all_to_all(pair, CHIPS, split_axis=0, concat_axis=0, tiled=True)
    group_sums, scores = total(arrived, 32)
    top = leaders(scores, lax.ppermute(scores, CORE, SWAP))
    return group_sums, top.reshape(TOPK)


def solution(mesh):
    finer = Mesh(mesh.devices.reshape(mesh.shape["section"], 4, 4, 2), DEVICES)
    return jax.shard_map(
        on_device,
        mesh=finer,
        in_specs=(
            P(DEVICES, None),
            P(None, DEVICES),
            P(),
            P(DEVICES),
            P(DEVICES, None),
            P(DEVICES),
            P(DEVICES),
            P(DEVICES, None),
        ),
        out_specs=(P(DEVICES, None), P()),
        check_vma=False,
    )
```

```python
import jax
import jax.numpy as jnp
from jax import lax
from jax.experimental import pallas as pl
from jax.experimental.pallas import tpu as pltpu
from jax.sharding import Mesh
from jax.sharding import PartitionSpec as P

BLOCK = 128
TOPK = 16
SLOTS = 64
DESTS = 128
AREA = 66
FLAT = DESTS * AREA
ROWS = DESTS * SLOTS
PIECES = 4
SPAN = 1024
BF = jnp.bfloat16
F32 = jnp.float32
I32 = jnp.int32
NT = (((1,), (1,)), ((), ()))
VMEM = pl.BlockSpec(memory_space=pltpu.VMEM)
SMEM = pl.BlockSpec(memory_space=pltpu.SMEM)
HBM = pl.BlockSpec(memory_space=pltpu.HBM)


def pack_kernel(
    bounds_hbm, lengths_hbm, measures_hbm, preds_hbm, dest_hbm, keys_hbm, groups_hbm, out_hbm,
    bounds_ref, lengths_ref, measures_ref, preds_ref, dest_ref, keys_ref, groups_ref,
    area_ref, area16_ref, place_ref, place_smem, sems,
):
    rows = measures_ref.shape[0]
    wide = 2 * BLOCK
    sources = (preds_hbm, dest_hbm, keys_hbm, groups_hbm, bounds_hbm, lengths_hbm, measures_hbm)
    targets = (preds_ref, dest_ref, keys_ref, groups_ref, bounds_ref, lengths_ref, measures_ref)
    loads = [
        pltpu.make_async_copy(source, target, sems.at[n])
        for n, (source, target) in enumerate(zip(sources, targets))
    ]
    for load in loads:
        load.start()

    def clear(i, _):
        area_ref[pl.ds(pl.multiple_of(i * 64, 64), 64), :] = jnp.zeros((64, BLOCK), F32)
        return 0

    lax.fori_loop(0, FLAT // 64, clear, 0, unroll=4)
    for load in loads[:-1]:
        load.wait()
    lane = lax.broadcasted_iota(I32, (1, BLOCK), 1)
    before = (
        lax.broadcasted_iota(I32, (wide, wide), 0) < lax.broadcasted_iota(I32, (wide, wide), 1)
    ).astype(F32).astype(BF)
    count_of = jnp.concatenate([before, jnp.ones((wide, wide), BF)], axis=1)
    dest_ids = lax.broadcasted_iota(I32, (DESTS, wide), 0)
    slot_ids = lax.broadcasted_iota(I32, (SLOTS, wide), 0)
    carry = jnp.zeros((DESTS, wide), F32)
    packed = jnp.zeros((DESTS, 4 * SLOTS), F32)

    def pair(ref, step):
        return jnp.concatenate(
            [ref[2 * step : 2 * step + 1, :], ref[2 * step + 1 : 2 * step + 2, :]], axis=1
        )

    for step in range(rows // wide):
        at = pl.ds(step * wide, wide)
        ok = jnp.concatenate([lane < lengths_ref[2 * step], lane < lengths_ref[2 * step + 1]], axis=1)
        for c in range(preds_ref.shape[0]):
            v = preds_ref[c : c + 1, at]
            ok = ok & (v >= bounds_ref[c, 0]) & (v < bounds_ref[c, 1])
        target = jnp.where(ok, pair(dest_ref, step), -1)
        keys = pair(keys_ref, step)
        groups = pair(groups_ref, step)
        names = (dest_ids == target).astype(F32)
        names16 = names.astype(BF)
        counts = jnp.dot(names16, count_of, preferred_element_type=F32)
        slot = jnp.sum(names * (counts[:, :wide] + carry), axis=0, keepdims=True).astype(I32)
        carry = carry + counts[:, wide:]
        place = jnp.where(ok, target * AREA + slot, FLAT)
        place_ref[2 * step : 2 * step + 1, :] = place[:, :BLOCK]
        place_ref[2 * step + 1 : 2 * step + 2, :] = place[:, BLOCK:]
        mine = slot_ids == slot
        values = [
            jnp.where(mine, part.astype(F32), 0.0).astype(BF)
            for part in ((keys >> 8) + 1, keys & 255, groups >> 8, groups & 255)
        ]
        packed = packed + lax.dot_general(
            names16, jnp.concatenate(values, axis=0), NT, preferred_element_type=F32
        )
    copy = pltpu.make_async_copy(place_ref, place_smem, sems.at[len(loads)])
    copy.start()
    for d in range(DESTS):
        area_ref[d * AREA + SLOTS : d * AREA + SLOTS + 1, :] = packed[d : d + 1, :BLOCK]
        area_ref[d * AREA + SLOTS + 1 : d * AREA + SLOTS + 2, :] = packed[d : d + 1, BLOCK:]
    loads[-1].wait()
    copy.wait()

    def put(b, _):
        for k in range(BLOCK // 16):
            x = measures_ref[pl.ds(pl.multiple_of(b * BLOCK + k * 16, 16), 16), :].astype(F32)
            for u in range(16):
                area_ref[pl.ds(place_smem[b, k * 16 + u], 1), :] = x[u : u + 1, :]
        return 0

    lax.fori_loop(0, rows // BLOCK, put, 0)

    def give(i, _):
        at = pl.ds(pl.multiple_of(i * 64, 64), 64)
        area16_ref[at, :] = area_ref[at, :].astype(BF)
        return 0

    stores = []
    part = FLAT // PIECES
    for n in range(PIECES):
        lax.fori_loop(n * part // 64, (n + 1) * part // 64, give, 0, unroll=3)
        at = pl.ds(n * part, part)
        stores.append(pltpu.make_async_copy(area16_ref.at[at], out_hbm.at[at], sems.at[8 + n]))
        stores[-1].start()
    for store in stores:
        store.wait()


def pack(bounds, lengths, measures, preds, dest, keys, groups):
    rows = measures.shape[0]
    blocks = rows // BLOCK
    return pl.pallas_call(
        pack_kernel,
        out_shape=jax.ShapeDtypeStruct((FLAT, BLOCK), BF),
        in_specs=[HBM] * 7,
        out_specs=HBM,
        scratch_shapes=[
            pltpu.SMEM(bounds.shape, I32),
            pltpu.SMEM(lengths.shape, I32),
            pltpu.VMEM(measures.shape, BF),
            pltpu.VMEM(preds.shape, I32),
            pltpu.VMEM((blocks, BLOCK), I32),
            pltpu.VMEM((blocks, BLOCK), I32),
            pltpu.VMEM((blocks, BLOCK), I32),
            pltpu.VMEM((FLAT + 8, BLOCK), F32),
            pltpu.VMEM((FLAT, BLOCK), BF),
            pltpu.VMEM((blocks, BLOCK), I32),
            pltpu.SMEM((blocks, BLOCK), I32),
            pltpu.SemaphoreType.DMA((8 + PIECES,)),
        ],
        compiler_params=pltpu.CompilerParams(vmem_limit_bytes=58 << 20),
        name="pack",
    )(bounds, lengths, measures, preds, dest, keys, groups)


def join_kernel(
    me_ref, got_ref, table_ref, own_ref, other_ref,
    pay_ref, side_ref, aux_ref, turned_ref, base_ref, base_smem, pair_ref, sums_ref, sem,
):
    for s in range(DESTS):
        pair = got_ref[s * AREA + SLOTS : (s + 1) * AREA, :].astype(F32)
        aux_ref[:, s : s + 1, :] = pair.reshape(2, 1, BLOCK)
    key_hi = aux_ref[0, :, :SLOTS]
    live = (key_hi > 0.0).astype(F32).astype(BF)
    counts = lax.dot_general(jnp.ones((8, SLOTS), BF), live, NT, preferred_element_type=F32)
    earlier = (
        lax.broadcasted_iota(I32, (DESTS, DESTS), 0) < lax.broadcasted_iota(I32, (DESTS, DESTS), 1)
    ).astype(F32).astype(BF)
    starts = jnp.dot(counts.astype(BF), earlier, preferred_element_type=F32)
    row = lax.broadcasted_iota(I32, (8, DESTS), 0)
    base_ref[...] = jnp.where(row == 0, starts, starts + counts).astype(I32)
    copy = pltpu.make_async_copy(base_ref, base_smem, sem)
    copy.start()
    key = (key_hi - 1.0) * 256.0 + aux_ref[0, :, SLOTS:]
    group = aux_ref[1, :, :SLOTS] * 256.0 + aux_ref[1, :, SLOTS:]
    code = key * 4096.0 + group
    turned_ref[...] = jnp.concatenate([code, code], axis=1).T
    sums_ref[...] = jnp.zeros_like(sums_ref)
    copy.wait()
    total = base_smem[1, DESTS - 1]
    for s in range(DESTS):
        at = pl.ds(base_smem[0, s], SLOTS)
        pay_ref[at, :] = got_ref[s * AREA : s * AREA + SLOTS, :].astype(F32)
        side_ref[at, :] = jnp.broadcast_to(turned_ref[:SLOTS, s : s + 1], (SLOTS, BLOCK))
    tab = jnp.concatenate([table_ref[:1024, :], table_ref[1024:, :]], axis=1)
    ids = lax.broadcasted_iota(I32, (BLOCK, 256), 1).astype(F32).astype(BF)
    rows_at = lax.broadcasted_iota(I32, (256, BLOCK), 0).astype(F32).astype(BF)
    spot = lax.broadcasted_iota(I32, (BLOCK, BLOCK), 0)
    one = jnp.ones((), BF)
    zero = jnp.zeros((), BF)

    def block(start, span):
        lows = []
        for n in range(span // BLOCK):
            first = pl.multiple_of(start + n * BLOCK, BLOCK)
            side = side_ref[pl.ds(first, BLOCK), :]
            key = jnp.floor(side * (1.0 / 4096.0))
            high = side - key * 4096.0 >= 2048.0
            group = side.T[:1, :]
            group = group - jnp.floor(group * (1.0 / 4096.0)) * 4096.0
            lows.append(jnp.where(group >= 2048.0, group - 2048.0, group))
            upper = key >= 1024.0
            key = jnp.where(upper, key - 1024.0, key)
            cols = []
            for t in range(4):
                k = (key - 256.0 * t).astype(BF)
                k = jnp.concatenate([k, k], axis=1)
                cols.append(jnp.where(ids == k, one, zero))
            found = jnp.dot(jnp.concatenate(cols, axis=1), tab, preferred_element_type=F32)
            found = jnp.where(upper, found[:, BLOCK:], found[:, :BLOCK])
            joined = pay_ref[pl.ds(first, BLOCK), :] * found
            none = jnp.zeros_like(joined)
            joined = jnp.where(first + spot < total, joined, none)
            to = pl.ds(n * BLOCK, BLOCK)
            pair_ref[to, :BLOCK] = jnp.where(high, none, joined).astype(BF)
            pair_ref[to, BLOCK:] = jnp.where(high, joined, none).astype(BF)
        for t in range(8):
            cols = [
                jnp.where(
                    rows_at == jnp.broadcast_to((low - 256.0 * t).astype(BF), (256, BLOCK)), one, zero
                )
                for low in lows
            ]
            at = pl.ds(t * 256, 256)
            sums_ref[at, :] += jnp.dot(
                jnp.concatenate(cols, axis=1), pair_ref[:span, :], preferred_element_type=F32
            )

    wide = total // SPAN * SPAN

    def wide_block(b, _):
        block(b * SPAN, SPAN)
        return 0

    def narrow_block(b, _):
        block(wide + b * (SPAN // 2), SPAN // 2)
        return 0

    lax.fori_loop(0, total // SPAN, wide_block, 0)
    lax.fori_loop(0, (total - wide + SPAN // 2 - 1) // (SPAN // 2), narrow_block, 0)
    me = me_ref[0]
    for i in range(64):
        col = (i // 32) * BLOCK
        base = (i % 32) * 64
        mine = pl.ds(pl.multiple_of(base + me * 32, 8), 32)
        theirs = pl.ds(pl.multiple_of(base + (1 - me) * 32, 8), 32)
        own_ref[i] = sums_ref[mine, col : col + BLOCK]
        other_ref[i] = sums_ref[theirs, col : col + BLOCK].astype(BF)


def join(me, got, table):
    return pl.pallas_call(
        join_kernel,
        out_shape=(
            jax.ShapeDtypeStruct((64, 32, BLOCK), F32),
            jax.ShapeDtypeStruct((64, 32, BLOCK), BF),
        ),
        in_specs=[SMEM, VMEM, VMEM],
        out_specs=(VMEM, VMEM),
        scratch_shapes=[
            pltpu.VMEM((ROWS, BLOCK), F32),
            pltpu.VMEM((ROWS, BLOCK), F32),
            pltpu.VMEM((2, DESTS, BLOCK), F32),
            pltpu.VMEM((BLOCK, BLOCK), F32),
            pltpu.VMEM((8, DESTS), I32),
            pltpu.SMEM((8, DESTS), I32),
            pltpu.VMEM((SPAN, 2 * BLOCK), BF),
            pltpu.VMEM((2048, 2 * BLOCK), F32),
            pltpu.SemaphoreType.DMA,
        ],
        compiler_params=pltpu.CompilerParams(vmem_limit_bytes=40 << 20),
        name="join",
    )(me, got, table)


def merge_kernel(own_ref, got_ref, out_ref):
    chips, rows, _ = own_ref.shape
    total = (own_ref[...] + got_ref[...].astype(F32)).astype(BF)
    out_ref[:, :rows, :] = total
    ones = jnp.ones((8, BLOCK), BF)
    flat = total.reshape(chips * rows, BLOCK)
    means = lax.dot_general(ones, flat, NT, preferred_element_type=F32)
    score = jnp.concatenate(
        [means[0:1, n * BLOCK : (n + 1) * BLOCK] for n in range(chips * rows // BLOCK)], axis=0
    )
    score = (score * (1.0 / BLOCK)).astype(BF)
    out_ref[:, rows:, :] = jnp.broadcast_to(score[None], (chips, *score.shape))


def merge(own, got):
    chips, rows, _ = own.shape
    return pl.pallas_call(
        merge_kernel,
        out_shape=jax.ShapeDtypeStruct((chips, rows + chips * rows // BLOCK, BLOCK), BF),
        in_specs=[VMEM, VMEM],
        out_specs=VMEM,
        compiler_params=pltpu.CompilerParams(vmem_limit_bytes=16 << 20),
        name="merge",
    )(own, got)


def total_kernel(got_ref, sums_ref, score_ref):
    rows = sums_ref.shape[0]
    total = got_ref[0].astype(F32)
    for p in range(1, got_ref.shape[0]):
        total = total + got_ref[p].astype(F32)
    sums_ref[...] = total[:rows, :]
    score_ref[...] = total[rows:, :]


def total(got, rows):
    return pl.pallas_call(
        total_kernel,
        out_shape=(
            jax.ShapeDtypeStruct((rows, BLOCK), F32),
            jax.ShapeDtypeStruct((got.shape[1] - rows, BLOCK), F32),
        ),
        in_specs=[VMEM],
        out_specs=(VMEM, VMEM),
        compiler_params=pltpu.CompilerParams(vmem_limit_bytes=8 << 20),
        name="total",
    )(got)


def leaders_kernel(a_ref, b_ref, out_ref):
    x = jnp.concatenate([a_ref[...], b_ref[...]], axis=0)
    lane = lax.broadcasted_iota(I32, (1, BLOCK), 1)
    taken = jnp.zeros((1, 1), F32)
    out = jnp.full((1, BLOCK), -jnp.inf, F32)
    place = lane.astype(F32)
    for _ in range(TOPK):
        best = jnp.max(jnp.max(x, axis=0, keepdims=True), axis=1, keepdims=True)
        same = x == best
        count = jnp.sum(
            jnp.sum(same.astype(F32), axis=0, keepdims=True), axis=1, keepdims=True
        )
        out = jnp.where((place >= taken) & (place < taken + count), best, out)
        taken = taken + count
        x = jnp.where(same, -jnp.inf, x)
    out_ref[...] = out[:, :TOPK]


def leaders(a, b):
    return pl.pallas_call(
        leaders_kernel,
        out_shape=jax.ShapeDtypeStruct((1, TOPK), F32),
        in_specs=[VMEM, VMEM],
        out_specs=VMEM,
        compiler_params=pltpu.CompilerParams(vmem_limit_bytes=4 << 20),
        name="leaders",
    )(a, b)


CHIPS = ("section", "dom_0", "dom_1")
CORE = "dom_2"
DEVICES = (*CHIPS, CORE)
SWAP = [(0, 1), (1, 0)]


def on_device(
    measures, pred_columns, bounds, lengths, destination, key_offset, group_ids, build_table
):
    blocks = measures.shape[0] // BLOCK
    me = lax.axis_index(CORE).astype(I32).reshape(1)

    def lanes(v):
        return v.reshape(blocks, BLOCK)

    me, bounds = lax.optimization_barrier((me, bounds))
    packets = pack(
        bounds, lengths, measures, pred_columns, lanes(destination), lanes(key_offset), lanes(group_ids)
    )
    got = lax.all_to_all(
        packets.reshape(DESTS, AREA // 2, 2, BLOCK), DEVICES, split_axis=0, concat_axis=0, tiled=True
    ).reshape(FLAT, BLOCK)
    mine, theirs = join(me, got, build_table)
    pair = merge(mine, lax.ppermute(theirs, CORE, SWAP))
    arrived = lax.all_to_all(pair, CHIPS, split_axis=0, concat_axis=0, tiled=True)
    group_sums, scores = total(arrived, 32)
    top = leaders(scores, lax.ppermute(scores, CORE, SWAP))
    return group_sums, top.reshape(TOPK)


def solution(mesh):
    finer = Mesh(mesh.devices.reshape(mesh.shape["section"], 4, 4, 2), DEVICES)
    return jax.shard_map(
        on_device,
        mesh=finer,
        in_specs=(
            P(DEVICES, None),
            P(None, DEVICES),
            P(),
            P(DEVICES),
            P(DEVICES, None),
            P(DEVICES),
            P(DEVICES),
            P(DEVICES, None),
        ),
        out_specs=(P(DEVICES, None), P()),
        check_vma=False,
    )
```

```python
import jax
import jax.numpy as jnp
from jax import lax
from jax.experimental import pallas as pl
from jax.experimental.pallas import tpu as pltpu
from jax.sharding import Mesh
from jax.sharding import PartitionSpec as P

BLOCK = 128
TOPK = 16
SLOTS = 64
DESTS = 128
AREA = 66
FLAT = DESTS * AREA
PIECES = 4
BF = jnp.bfloat16
F32 = jnp.float32
I32 = jnp.int32
NT = (((1,), (1,)), ((), ()))
VMEM = pl.BlockSpec(memory_space=pltpu.VMEM)
SMEM = pl.BlockSpec(memory_space=pltpu.SMEM)
HBM = pl.BlockSpec(memory_space=pltpu.HBM)


def pack_kernel(
    bounds_hbm, lengths_hbm, measures_hbm, preds_hbm, dest_hbm, keys_hbm, groups_hbm, out_hbm,
    bounds_ref, lengths_ref, measures_ref, preds_ref, dest_ref, keys_ref, groups_ref,
    area_ref, area16_ref, place_ref, place_smem, sems,
):
    rows = measures_ref.shape[0]
    wide = 2 * BLOCK
    sources = (preds_hbm, dest_hbm, keys_hbm, groups_hbm, bounds_hbm, lengths_hbm, measures_hbm)
    targets = (preds_ref, dest_ref, keys_ref, groups_ref, bounds_ref, lengths_ref, measures_ref)
    loads = [
        pltpu.make_async_copy(source, target, sems.at[n])
        for n, (source, target) in enumerate(zip(sources, targets))
    ]
    for load in loads:
        load.start()

    def clear(i, _):
        area_ref[pl.ds(pl.multiple_of(i * 64, 64), 64), :] = jnp.zeros((64, BLOCK), F32)
        return 0

    lax.fori_loop(0, FLAT // 64, clear, 0, unroll=4)
    for load in loads[:-1]:
        load.wait()
    lane = lax.broadcasted_iota(I32, (1, BLOCK), 1)
    before = (
        lax.broadcasted_iota(I32, (wide, wide), 0) < lax.broadcasted_iota(I32, (wide, wide), 1)
    ).astype(F32).astype(BF)
    count_of = jnp.concatenate([before, jnp.ones((wide, wide), BF)], axis=1)
    dest_ids = lax.broadcasted_iota(I32, (DESTS, wide), 0)
    slot_ids = lax.broadcasted_iota(I32, (SLOTS, wide), 0)
    carry = jnp.zeros((DESTS, wide), F32)
    packed = jnp.zeros((DESTS, 4 * SLOTS), F32)

    def pair(ref, step):
        return jnp.concatenate(
            [ref[2 * step : 2 * step + 1, :], ref[2 * step + 1 : 2 * step + 2, :]], axis=1
        )

    for step in range(rows // wide):
        at = pl.ds(step * wide, wide)
        ok = jnp.concatenate([lane < lengths_ref[2 * step], lane < lengths_ref[2 * step + 1]], axis=1)
        for c in range(preds_ref.shape[0]):
            v = preds_ref[c : c + 1, at]
            ok = ok & (v >= bounds_ref[c, 0]) & (v < bounds_ref[c, 1])
        target = jnp.where(ok, pair(dest_ref, step), -1)
        keys = pair(keys_ref, step)
        groups = pair(groups_ref, step)
        names = (dest_ids == target).astype(F32)
        names16 = names.astype(BF)
        counts = jnp.dot(names16, count_of, preferred_element_type=F32)
        slot = jnp.sum(names * (counts[:, :wide] + carry), axis=0, keepdims=True).astype(I32)
        carry = carry + counts[:, wide:]
        place = jnp.where(ok, target * AREA + slot, FLAT)
        place_ref[2 * step : 2 * step + 1, :] = place[:, :BLOCK]
        place_ref[2 * step + 1 : 2 * step + 2, :] = place[:, BLOCK:]
        mine = slot_ids == slot
        values = [
            jnp.where(mine, part.astype(F32), 0.0).astype(BF)
            for part in (keys >> 8, keys & 255, groups >> 8, groups & 255)
        ]
        packed = packed + lax.dot_general(
            names16, jnp.concatenate(values, axis=0), NT, preferred_element_type=F32
        )
    copy = pltpu.make_async_copy(place_ref, place_smem, sems.at[len(loads)])
    copy.start()
    for d in range(DESTS):
        area_ref[d * AREA + SLOTS : d * AREA + SLOTS + 1, :] = packed[d : d + 1, :BLOCK]
        area_ref[d * AREA + SLOTS + 1 : d * AREA + SLOTS + 2, :] = packed[d : d + 1, BLOCK:]
    loads[-1].wait()
    copy.wait()

    def put(b, _):
        for k in range(BLOCK // 16):
            x = measures_ref[pl.ds(pl.multiple_of(b * BLOCK + k * 16, 16), 16), :].astype(F32)
            for u in range(16):
                area_ref[pl.ds(place_smem[b, k * 16 + u], 1), :] = x[u : u + 1, :]
        return 0

    lax.fori_loop(0, rows // BLOCK, put, 0)

    def give(i, _):
        at = pl.ds(pl.multiple_of(i * 64, 64), 64)
        area16_ref[at, :] = area_ref[at, :].astype(BF)
        return 0

    stores = []
    part = FLAT // PIECES
    for n in range(PIECES):
        lax.fori_loop(n * part // 64, (n + 1) * part // 64, give, 0, unroll=3)
        at = pl.ds(n * part, part)
        stores.append(pltpu.make_async_copy(area16_ref.at[at], out_hbm.at[at], sems.at[8 + n]))
        stores[-1].start()
    for store in stores:
        store.wait()


def pack(bounds, lengths, measures, preds, dest, keys, groups):
    rows = measures.shape[0]
    blocks = rows // BLOCK
    return pl.pallas_call(
        pack_kernel,
        out_shape=jax.ShapeDtypeStruct((FLAT, BLOCK), BF),
        in_specs=[HBM] * 7,
        out_specs=HBM,
        scratch_shapes=[
            pltpu.SMEM(bounds.shape, I32),
            pltpu.SMEM(lengths.shape, I32),
            pltpu.VMEM(measures.shape, BF),
            pltpu.VMEM(preds.shape, I32),
            pltpu.VMEM((blocks, BLOCK), I32),
            pltpu.VMEM((blocks, BLOCK), I32),
            pltpu.VMEM((blocks, BLOCK), I32),
            pltpu.VMEM((FLAT + 8, BLOCK), F32),
            pltpu.VMEM((FLAT, BLOCK), BF),
            pltpu.VMEM((blocks, BLOCK), I32),
            pltpu.SMEM((blocks, BLOCK), I32),
            pltpu.SemaphoreType.DMA((8 + PIECES,)),
        ],
        compiler_params=pltpu.CompilerParams(vmem_limit_bytes=58 << 20),
        name="pack",
    )(bounds, lengths, measures, preds, dest, keys, groups)


def join_kernel(me_ref, got_ref, table_ref, own_ref, other_ref, pair_ref, sums_ref, keyt_ref, group_ref, aux_ref):
    chips = DESTS // 2
    for d in range(DESTS):
        pair = got_ref[d * AREA + SLOTS : (d + 1) * AREA, :].astype(F32)
        aux_ref[:, d : d + 1, :] = pair.reshape(2, 1, BLOCK)
    ka, kb = aux_ref[0, :chips, :], aux_ref[0, chips:, :]
    ga, gb = aux_ref[1, :chips, :], aux_ref[1, chips:, :]

    def halves(a, b):
        return (
            jnp.concatenate([a[:, :SLOTS], b[:, :SLOTS]], axis=1),
            jnp.concatenate([a[:, SLOTS:], b[:, SLOTS:]], axis=1),
        )

    key_hi, key_lo = halves(ka, kb)
    grp_hi, grp_lo = halves(ga, gb)
    keyt_ref[...] = jnp.concatenate([key_hi * 256.0 + key_lo, grp_hi], axis=0).T
    group_ref[0] = grp_hi
    group_ref[1] = grp_lo
    tab = jnp.concatenate([table_ref[:1024, :], table_ref[1024:, :]], axis=1)
    ids = lax.broadcasted_iota(I32, (BLOCK, 256), 1).astype(F32).astype(BF)
    one = jnp.ones((), BF)
    zero = jnp.zeros((), BF)
    for p in range(chips):
        key = jnp.broadcast_to(keyt_ref[:, p : p + 1], (BLOCK, BLOCK))
        top = jnp.broadcast_to(keyt_ref[:, chips + p : chips + p + 1], (BLOCK, BLOCK))
        upper = key >= 1024.0
        key = jnp.where(upper, key - 1024.0, key)
        cols = []
        for t in range(4):
            k = (key - 256.0 * t).astype(BF)
            k = jnp.concatenate([k, k], axis=1)
            cols.append(jnp.where(ids == k, one, zero))
        found = jnp.dot(jnp.concatenate(cols, axis=1), tab, preferred_element_type=F32)
        row = jnp.where(upper, found[:, BLOCK:], found[:, :BLOCK])
        low, high_at = p * AREA, (chips + p) * AREA
        pay = jnp.concatenate(
            [got_ref[low : low + SLOTS, :], got_ref[high_at : high_at + SLOTS, :]], axis=0
        )
        joined = pay.astype(F32) * row
        high = top >= 8.0
        none = jnp.zeros_like(joined)
        pair_ref[p * BLOCK : (p + 1) * BLOCK, :BLOCK] = jnp.where(high, none, joined).astype(BF)
        pair_ref[p * BLOCK : (p + 1) * BLOCK, BLOCK:] = jnp.where(high, joined, none).astype(BF)

    rows_at = lax.broadcasted_iota(I32, (256, BLOCK), 0).astype(F32).astype(BF)
    per = 8
    for k in range(chips // per):
        low3 = []
        for p in range(k * per, (k + 1) * per):
            hi = group_ref[0, p : p + 1, :]
            low3.append((jnp.where(hi >= 8.0, hi - 8.0, hi), group_ref[1, p : p + 1, :]))
        block = pair_ref[k * per * BLOCK : (k + 1) * per * BLOCK, :]
        for t in range(8):
            cols = []
            for hi, lo in low3:
                v = jnp.where(hi == float(t), lo, -1.0).astype(BF)
                cols.append(jnp.where(rows_at == jnp.broadcast_to(v, (256, BLOCK)), one, zero))
            part = jnp.dot(jnp.concatenate(cols, axis=1), block, preferred_element_type=F32)
            at = pl.ds(t * 256, 256)
            if k == 0:
                sums_ref[at, :] = part
            else:
                sums_ref[at, :] = sums_ref[at, :] + part

    me = me_ref[0]
    for i in range(64):
        col = (i // 32) * BLOCK
        base = (i % 32) * 64
        mine = pl.ds(pl.multiple_of(base + me * 32, 8), 32)
        theirs = pl.ds(pl.multiple_of(base + (1 - me) * 32, 8), 32)
        own_ref[i] = sums_ref[mine, col : col + BLOCK]
        other_ref[i] = sums_ref[theirs, col : col + BLOCK].astype(BF)


def join(me, got, table):
    chips = DESTS // 2
    return pl.pallas_call(
        join_kernel,
        out_shape=(
            jax.ShapeDtypeStruct((chips, 32, BLOCK), F32),
            jax.ShapeDtypeStruct((chips, 32, BLOCK), BF),
        ),
        in_specs=[SMEM, VMEM, VMEM],
        out_specs=(VMEM, VMEM),
        scratch_shapes=[
            pltpu.VMEM((chips * BLOCK, 2 * BLOCK), BF),
            pltpu.VMEM((2048, 2 * BLOCK), F32),
            pltpu.VMEM((BLOCK, BLOCK), F32),
            pltpu.VMEM((2, chips, BLOCK), F32),
            pltpu.VMEM((2, DESTS, BLOCK), F32),
        ],
        compiler_params=pltpu.CompilerParams(vmem_limit_bytes=40 << 20),
        name="join",
    )(me, got, table)


def merge_kernel(own_ref, got_ref, out_ref):
    chips, rows, _ = own_ref.shape
    total = (own_ref[...] + got_ref[...].astype(F32)).astype(BF)
    out_ref[:, :rows, :] = total
    ones = jnp.ones((8, BLOCK), BF)
    flat = total.reshape(chips * rows, BLOCK)
    means = lax.dot_general(ones, flat, NT, preferred_element_type=F32)
    score = jnp.concatenate(
        [means[0:1, n * BLOCK : (n + 1) * BLOCK] for n in range(chips * rows // BLOCK)], axis=0
    )
    score = (score * (1.0 / BLOCK)).astype(BF)
    out_ref[:, rows:, :] = jnp.broadcast_to(score[None], (chips, *score.shape))


def merge(own, got):
    chips, rows, _ = own.shape
    return pl.pallas_call(
        merge_kernel,
        out_shape=jax.ShapeDtypeStruct((chips, rows + chips * rows // BLOCK, BLOCK), BF),
        in_specs=[VMEM, VMEM],
        out_specs=VMEM,
        compiler_params=pltpu.CompilerParams(vmem_limit_bytes=16 << 20),
        name="merge",
    )(own, got)


def total_kernel(got_ref, sums_ref, score_ref):
    rows = sums_ref.shape[0]
    total = got_ref[0].astype(F32)
    for p in range(1, got_ref.shape[0]):
        total = total + got_ref[p].astype(F32)
    sums_ref[...] = total[:rows, :]
    score_ref[...] = total[rows:, :]


def total(got, rows):
    return pl.pallas_call(
        total_kernel,
        out_shape=(
            jax.ShapeDtypeStruct((rows, BLOCK), F32),
            jax.ShapeDtypeStruct((got.shape[1] - rows, BLOCK), F32),
        ),
        in_specs=[VMEM],
        out_specs=(VMEM, VMEM),
        compiler_params=pltpu.CompilerParams(vmem_limit_bytes=8 << 20),
        name="total",
    )(got)


def leaders_kernel(a_ref, b_ref, out_ref):
    x = jnp.concatenate([a_ref[...], b_ref[...]], axis=0)
    lane = lax.broadcasted_iota(I32, (1, BLOCK), 1)
    taken = jnp.zeros((1, 1), F32)
    out = jnp.full((1, BLOCK), -jnp.inf, F32)
    place = lane.astype(F32)
    for _ in range(TOPK):
        best = jnp.max(jnp.max(x, axis=0, keepdims=True), axis=1, keepdims=True)
        same = x == best
        count = jnp.sum(
            jnp.sum(same.astype(F32), axis=0, keepdims=True), axis=1, keepdims=True
        )
        out = jnp.where((place >= taken) & (place < taken + count), best, out)
        taken = taken + count
        x = jnp.where(same, -jnp.inf, x)
    out_ref[...] = out[:, :TOPK]


def leaders(a, b):
    return pl.pallas_call(
        leaders_kernel,
        out_shape=jax.ShapeDtypeStruct((1, TOPK), F32),
        in_specs=[VMEM, VMEM],
        out_specs=VMEM,
        compiler_params=pltpu.CompilerParams(vmem_limit_bytes=4 << 20),
        name="leaders",
    )(a, b)


CHIPS = ("section", "dom_0", "dom_1")
CORE = "dom_2"
DEVICES = (*CHIPS, CORE)
SWAP = [(0, 1), (1, 0)]


def on_device(
    measures, pred_columns, bounds, lengths, destination, key_offset, group_ids, build_table
):
    blocks = measures.shape[0] // BLOCK
    me = lax.axis_index(CORE).astype(I32).reshape(1)

    def lanes(v):
        return v.reshape(blocks, BLOCK)

    me, bounds = lax.optimization_barrier((me, bounds))
    packets = pack(
        bounds, lengths, measures, pred_columns, lanes(destination), lanes(key_offset), lanes(group_ids)
    )
    got = lax.all_to_all(
        packets.reshape(DESTS, AREA // 2, 2, BLOCK), DEVICES, split_axis=0, concat_axis=0, tiled=True
    ).reshape(FLAT, BLOCK)
    mine, theirs = join(me, got, build_table)
    pair = merge(mine, lax.ppermute(theirs, CORE, SWAP))
    arrived = lax.all_to_all(pair, CHIPS, split_axis=0, concat_axis=0, tiled=True)
    group_sums, scores = total(arrived, 32)
    top = leaders(scores, lax.ppermute(scores, CORE, SWAP))
    return group_sums, top.reshape(TOPK)


def solution(mesh):
    finer = Mesh(mesh.devices.reshape(mesh.shape["section"], 4, 4, 2), DEVICES)
    return jax.shard_map(
        on_device,
        mesh=finer,
        in_specs=(
            P(DEVICES, None),
            P(None, DEVICES),
            P(),
            P(DEVICES),
            P(DEVICES, None),
            P(DEVICES),
            P(DEVICES),
            P(DEVICES, None),
        ),
        out_specs=(P(DEVICES, None), P()),
        check_vma=False,
    )
```

```python
import jax
import jax.numpy as jnp
from jax import lax
from jax.experimental import pallas as pl
from jax.experimental.pallas import tpu as pltpu
from jax.sharding import Mesh
from jax.sharding import PartitionSpec as P

BLOCK = 128
TOPK = 16
SLOTS = 64
DESTS = 128
AREA = 66
FLAT = DESTS * AREA
PIECES = 4
PER = 8
TILES = 2
FETCH = 2
BF = jnp.bfloat16
F32 = jnp.float32
I32 = jnp.int32
NT = (((1,), (1,)), ((), ()))
VMEM = pl.BlockSpec(memory_space=pltpu.VMEM)
SMEM = pl.BlockSpec(memory_space=pltpu.SMEM)
HBM = pl.BlockSpec(memory_space=pltpu.HBM)


def group_code(g):
    high = ((g >> 11) << 3) + (((g >> 5) & 1) << 2) + ((g >> 9) & 3)
    return high, (((g >> 6) & 7) << 5) + (g & 31)


def pack_kernel(
    bounds_hbm, lengths_hbm, measures_hbm, preds_hbm, dest_hbm, keys_hbm, groups_hbm, out_hbm,
    bounds_ref, lengths_ref, measures_ref, preds_ref, dest_ref, keys_ref, groups_ref,
    area_ref, area16_ref, place_ref, place_smem, sems,
):
    rows = measures_ref.shape[0]
    wide = 2 * BLOCK
    sources = (preds_hbm, dest_hbm, keys_hbm, groups_hbm, bounds_hbm, lengths_hbm, measures_hbm)
    targets = (preds_ref, dest_ref, keys_ref, groups_ref, bounds_ref, lengths_ref, measures_ref)
    loads = [
        pltpu.make_async_copy(source, target, sems.at[n])
        for n, (source, target) in enumerate(zip(sources, targets))
    ]
    for load in loads:
        load.start()

    def clear(i, _):
        area_ref[pl.ds(pl.multiple_of(i * 64, 64), 64), :] = jnp.zeros((64, BLOCK), F32)
        return 0

    lax.fori_loop(0, FLAT // 64, clear, 0, unroll=4)
    for load in loads[:-1]:
        load.wait()
    lane = lax.broadcasted_iota(I32, (1, BLOCK), 1)
    before = (
        lax.broadcasted_iota(I32, (wide, wide), 0) < lax.broadcasted_iota(I32, (wide, wide), 1)
    ).astype(F32).astype(BF)
    count_of = jnp.concatenate([before, jnp.ones((wide, wide), BF)], axis=1)
    dest_ids = lax.broadcasted_iota(I32, (DESTS, wide), 0)
    slot_ids = lax.broadcasted_iota(I32, (SLOTS, wide), 0)
    carry = jnp.zeros((DESTS, wide), F32)
    packed = jnp.zeros((DESTS, 4 * SLOTS), F32)

    def pair(ref, step):
        return jnp.concatenate(
            [ref[2 * step : 2 * step + 1, :], ref[2 * step + 1 : 2 * step + 2, :]], axis=1
        )

    for step in range(rows // wide):
        at = pl.ds(step * wide, wide)
        ok = jnp.concatenate([lane < lengths_ref[2 * step], lane < lengths_ref[2 * step + 1]], axis=1)
        for c in range(preds_ref.shape[0]):
            v = preds_ref[c : c + 1, at]
            ok = ok & (v >= bounds_ref[c, 0]) & (v < bounds_ref[c, 1])
        target = jnp.where(ok, pair(dest_ref, step), -1)
        keys = pair(keys_ref, step)
        groups = pair(groups_ref, step)
        names = (dest_ids == target).astype(F32)
        names16 = names.astype(BF)
        counts = jnp.dot(names16, count_of, preferred_element_type=F32)
        slot = jnp.sum(names * (counts[:, :wide] + carry), axis=0, keepdims=True).astype(I32)
        carry = carry + counts[:, wide:]
        place = jnp.where(ok, target * AREA + slot, FLAT)
        place_ref[2 * step : 2 * step + 1, :] = place[:, :BLOCK]
        place_ref[2 * step + 1 : 2 * step + 2, :] = place[:, BLOCK:]
        mine = slot_ids == slot
        values = [
            jnp.where(mine, part.astype(F32), 0.0).astype(BF)
            for part in (keys >> 8, keys & 255, *group_code(groups))
        ]
        packed = packed + lax.dot_general(
            names16, jnp.concatenate(values, axis=0), NT, preferred_element_type=F32
        )
    copy = pltpu.make_async_copy(place_ref, place_smem, sems.at[len(loads)])
    copy.start()
    for d in range(DESTS):
        area_ref[d * AREA + SLOTS : d * AREA + SLOTS + 1, :] = packed[d : d + 1, :BLOCK]
        area_ref[d * AREA + SLOTS + 1 : d * AREA + SLOTS + 2, :] = packed[d : d + 1, BLOCK:]
    loads[-1].wait()
    copy.wait()

    def put(b, _):
        for k in range(BLOCK // 16):
            x = measures_ref[pl.ds(pl.multiple_of(b * BLOCK + k * 16, 16), 16), :].astype(F32)
            for u in range(16):
                area_ref[pl.ds(place_smem[b, k * 16 + u], 1), :] = x[u : u + 1, :]
        return 0

    lax.fori_loop(0, rows // BLOCK, put, 0)

    def give(i, _):
        at = pl.ds(pl.multiple_of(i * 64, 64), 64)
        area16_ref[at, :] = area_ref[at, :].astype(BF)
        return 0

    stores = []
    part = FLAT // PIECES
    for n in range(PIECES):
        lax.fori_loop(n * part // 64, (n + 1) * part // 64, give, 0, unroll=3)
        at = pl.ds(n * part, part)
        stores.append(pltpu.make_async_copy(area16_ref.at[at], out_hbm.at[at], sems.at[8 + n]))
        stores[-1].start()
    for store in stores:
        store.wait()


def pack(bounds, lengths, measures, preds, dest, keys, groups):
    rows = measures.shape[0]
    blocks = rows // BLOCK
    return pl.pallas_call(
        pack_kernel,
        out_shape=jax.ShapeDtypeStruct((FLAT, BLOCK), BF),
        in_specs=[HBM] * 7,
        out_specs=HBM,
        scratch_shapes=[
            pltpu.SMEM(bounds.shape, I32),
            pltpu.SMEM(lengths.shape, I32),
            pltpu.VMEM(measures.shape, BF),
            pltpu.VMEM(preds.shape, I32),
            pltpu.VMEM((blocks, BLOCK), I32),
            pltpu.VMEM((blocks, BLOCK), I32),
            pltpu.VMEM((blocks, BLOCK), I32),
            pltpu.VMEM((FLAT + 8, BLOCK), F32),
            pltpu.VMEM((FLAT, BLOCK), BF),
            pltpu.VMEM((blocks, BLOCK), I32),
            pltpu.SMEM((blocks, BLOCK), I32),
            pltpu.SemaphoreType.DMA((8 + PIECES,)),
        ],
        compiler_params=pltpu.CompilerParams(vmem_limit_bytes=58 << 20),
        name="pack",
    )(bounds, lengths, measures, preds, dest, keys, groups)


def add_groups(core, group_ref, pair_ref, sums_ref):
    rows_at = lax.broadcasted_iota(I32, (256, BLOCK), 0).astype(F32).astype(BF)
    one = jnp.ones((), BF)
    zero = jnp.zeros((), BF)
    first = (core * 4).astype(F32)
    for k in range(DESTS // 2 // PER):
        lows = []
        for p in range(k * PER, (k + 1) * PER):
            hi = group_ref[0, p : p + 1, :]
            lows.append((jnp.where(hi >= 8.0, hi - 8.0, hi) - first, group_ref[1, p : p + 1, :]))
        block = pair_ref[k * PER * BLOCK : (k + 1) * PER * BLOCK, :]
        for t in range(0, 4, TILES):
            tiles = []
            for u in range(t, t + TILES):
                cols = []
                for hi, lo in lows:
                    v = jnp.where(hi == float(u), lo, -1.0).astype(BF)
                    cols.append(jnp.where(rows_at == jnp.broadcast_to(v, (256, BLOCK)), one, zero))
                tiles.append(jnp.concatenate(cols, axis=1))
            part = jnp.dot(jnp.concatenate(tiles, axis=0), block, preferred_element_type=F32)
            at = pl.ds(t * 256, TILES * 256)
            if k == 0:
                sums_ref[at, :] = part
            else:
                sums_ref[at, :] = sums_ref[at, :] + part


def join_kernel(me_ref, got_ref, table_ref, other_ref, pair_ref, group_ref, sums_ref, turned_ref, aux_ref):
    blocks = DESTS // 2
    for d in range(DESTS):
        pair = got_ref[d * AREA + SLOTS : (d + 1) * AREA, :].astype(F32)
        aux_ref[:, d : d + 1, :] = pair.reshape(2, 1, BLOCK)

    def halves(n):
        a, b = aux_ref[n, :blocks, :], aux_ref[n, blocks:, :]
        return (
            jnp.concatenate([a[:, :SLOTS], b[:, :SLOTS]], axis=1),
            jnp.concatenate([a[:, SLOTS:], b[:, SLOTS:]], axis=1),
        )

    key_hi, key_lo = halves(0)
    grp_hi, grp_lo = halves(1)
    turned_ref[...] = jnp.concatenate([key_hi * 256.0 + key_lo, grp_hi], axis=0).T
    group_ref[0] = grp_hi
    group_ref[1] = grp_lo
    tab = jnp.concatenate([table_ref[:1024, :], table_ref[1024:, :]], axis=1)
    ids = lax.broadcasted_iota(I32, (BLOCK, 256), 1).astype(F32).astype(BF)
    one = jnp.ones((), BF)
    zero = jnp.zeros((), BF)
    for q in range(0, blocks, FETCH):
        picks = []
        uppers = []
        for p in range(q, q + FETCH):
            key = jnp.broadcast_to(turned_ref[:, p : p + 1], (BLOCK, BLOCK))
            upper = key >= 1024.0
            uppers.append(upper)
            key = jnp.where(upper, key - 1024.0, key)
            cols = []
            for t in range(4):
                k = (key - 256.0 * t).astype(BF)
                k = jnp.concatenate([k, k], axis=1)
                cols.append(jnp.where(ids == k, one, zero))
            picks.append(jnp.concatenate(cols, axis=1))
        found = jnp.dot(jnp.concatenate(picks, axis=0), tab, preferred_element_type=F32)
        for p in range(q, q + FETCH):
            mine = found[(p - q) * BLOCK : (p - q + 1) * BLOCK, :]
            row = jnp.where(uppers[p - q], mine[:, BLOCK:], mine[:, :BLOCK])
            low, high_at = p * AREA, (blocks + p) * AREA
            pay = jnp.concatenate(
                [got_ref[low : low + SLOTS, :], got_ref[high_at : high_at + SLOTS, :]], axis=0
            )
            joined = pay.astype(F32) * row
            high = jnp.broadcast_to(turned_ref[:, blocks + p : blocks + p + 1], (BLOCK, BLOCK)) >= 8.0
            none = jnp.zeros_like(joined)
            to = slice(p * BLOCK, (p + 1) * BLOCK)
            pair_ref[to, :BLOCK] = jnp.where(high, none, joined).astype(BF)
            pair_ref[to, BLOCK:] = jnp.where(high, joined, none).astype(BF)
    add_groups(1 - me_ref[0], group_ref, pair_ref, sums_ref)
    for q in range(64):
        at = slice(q % 32 * 32, (q % 32 + 1) * 32)
        other_ref[q] = sums_ref[at, q // 32 * BLOCK : (q // 32 + 1) * BLOCK].astype(BF)


def join(me, got, table):
    blocks = DESTS // 2
    return pl.pallas_call(
        join_kernel,
        out_shape=(
            jax.ShapeDtypeStruct((64, 32, BLOCK), BF),
            jax.ShapeDtypeStruct((blocks * BLOCK, 2 * BLOCK), BF),
            jax.ShapeDtypeStruct((2, blocks, BLOCK), F32),
        ),
        in_specs=[SMEM, VMEM, VMEM],
        out_specs=(VMEM, VMEM, VMEM),
        scratch_shapes=[
            pltpu.VMEM((1024, 2 * BLOCK), F32),
            pltpu.VMEM((BLOCK, BLOCK), F32),
            pltpu.VMEM((2, DESTS, BLOCK), F32),
        ],
        cost_estimate=pl.CostEstimate(flops=9 << 30, bytes_accessed=8 << 20, transcendentals=0),
        compiler_params=pltpu.CompilerParams(vmem_limit_bytes=30 << 20),
        name="join",
    )(me, got, table)


def rest_kernel(me_ref, pair_ref, group_ref, own_ref, sums_ref):
    add_groups(me_ref[0], group_ref, pair_ref, sums_ref)
    for q in range(64):
        at = slice(q % 32 * 32, (q % 32 + 1) * 32)
        own_ref[q] = sums_ref[at, q // 32 * BLOCK : (q // 32 + 1) * BLOCK]


def rest(me, pair, group):
    return pl.pallas_call(
        rest_kernel,
        out_shape=jax.ShapeDtypeStruct((64, 32, BLOCK), F32),
        in_specs=[SMEM, VMEM, VMEM],
        out_specs=VMEM,
        scratch_shapes=[pltpu.VMEM((1024, 2 * BLOCK), F32)],
        cost_estimate=pl.CostEstimate(flops=5 << 30, bytes_accessed=8 << 20, transcendentals=0),
        compiler_params=pltpu.CompilerParams(vmem_limit_bytes=24 << 20),
        name="rest",
    )(me, pair, group)


def merge_kernel(own_ref, got_ref, out_ref):
    chips, rows, _ = own_ref.shape
    total = (own_ref[...] + got_ref[...].astype(F32)).astype(BF)
    out_ref[:, :rows, :] = total
    ones = jnp.ones((8, BLOCK), BF)
    flat = total.reshape(chips * rows, BLOCK)
    means = lax.dot_general(ones, flat, NT, preferred_element_type=F32)
    score = jnp.concatenate(
        [means[0:1, n * BLOCK : (n + 1) * BLOCK] for n in range(chips * rows // BLOCK)], axis=0
    )
    score = (score * (1.0 / BLOCK)).astype(BF)
    out_ref[:, rows:, :] = jnp.broadcast_to(score[None], (chips, *score.shape))


def merge(own, got):
    chips, rows, _ = own.shape
    return pl.pallas_call(
        merge_kernel,
        out_shape=jax.ShapeDtypeStruct((chips, rows + chips * rows // BLOCK, BLOCK), BF),
        in_specs=[VMEM, VMEM],
        out_specs=VMEM,
        compiler_params=pltpu.CompilerParams(vmem_limit_bytes=16 << 20),
        name="merge",
    )(own, got)


def total_kernel(got_ref, sums_ref, score_ref):
    rows = sums_ref.shape[0]
    total = got_ref[0].astype(F32)
    for p in range(1, got_ref.shape[0]):
        total = total + got_ref[p].astype(F32)
    sums_ref[...] = total[:rows, :]
    score_ref[...] = total[rows:, :]


def total(got, rows):
    return pl.pallas_call(
        total_kernel,
        out_shape=(
            jax.ShapeDtypeStruct((rows, BLOCK), F32),
            jax.ShapeDtypeStruct((got.shape[1] - rows, BLOCK), F32),
        ),
        in_specs=[VMEM],
        out_specs=(VMEM, VMEM),
        compiler_params=pltpu.CompilerParams(vmem_limit_bytes=8 << 20),
        name="total",
    )(got)


def leaders_kernel(a_ref, b_ref, out_ref):
    x = jnp.concatenate([a_ref[...], b_ref[...]], axis=0)
    lane = lax.broadcasted_iota(I32, (1, BLOCK), 1)
    taken = jnp.zeros((1, 1), F32)
    out = jnp.full((1, BLOCK), -jnp.inf, F32)
    place = lane.astype(F32)
    for _ in range(TOPK):
        best = jnp.max(jnp.max(x, axis=0, keepdims=True), axis=1, keepdims=True)
        same = x == best
        count = jnp.sum(
            jnp.sum(same.astype(F32), axis=0, keepdims=True), axis=1, keepdims=True
        )
        out = jnp.where((place >= taken) & (place < taken + count), best, out)
        taken = taken + count
        x = jnp.where(same, -jnp.inf, x)
    out_ref[...] = out[:, :TOPK]


def leaders(a, b):
    return pl.pallas_call(
        leaders_kernel,
        out_shape=jax.ShapeDtypeStruct((1, TOPK), F32),
        in_specs=[VMEM, VMEM],
        out_specs=VMEM,
        compiler_params=pltpu.CompilerParams(vmem_limit_bytes=4 << 20),
        name="leaders",
    )(a, b)


CHIPS = ("section", "dom_0", "dom_1")
CORE = "dom_2"
DEVICES = (*CHIPS, CORE)
SWAP = [(0, 1), (1, 0)]


def on_device(
    measures, pred_columns, bounds, lengths, destination, key_offset, group_ids, build_table
):
    blocks = measures.shape[0] // BLOCK
    me = lax.axis_index(CORE).astype(I32).reshape(1)

    def lanes(v):
        return v.reshape(blocks, BLOCK)

    me, bounds = lax.optimization_barrier((me, bounds))
    packets = pack(
        bounds, lengths, measures, pred_columns, lanes(destination), lanes(key_offset), lanes(group_ids)
    )
    got = lax.all_to_all(
        packets.reshape(DESTS, AREA // 2, 2, BLOCK), DEVICES, split_axis=0, concat_axis=0, tiled=True
    ).reshape(FLAT, BLOCK)
    theirs, joined, codes = join(me, got, build_table)
    from_partner = lax.ppermute(theirs, CORE, SWAP)
    pair = merge(rest(me, joined, codes), from_partner)
    arrived = lax.all_to_all(pair, CHIPS, split_axis=0, concat_axis=0, tiled=True)
    group_sums, scores = total(arrived, 32)
    top = leaders(scores, lax.ppermute(scores, CORE, SWAP))
    return group_sums, top.reshape(TOPK)


def solution(mesh):
    finer = Mesh(mesh.devices.reshape(mesh.shape["section"], 4, 4, 2), DEVICES)
    return jax.shard_map(
        on_device,
        mesh=finer,
        in_specs=(
            P(DEVICES, None),
            P(None, DEVICES),
            P(),
            P(DEVICES),
            P(DEVICES, None),
            P(DEVICES),
            P(DEVICES),
            P(DEVICES, None),
        ),
        out_specs=(P(DEVICES, None), P()),
        check_vma=False,
    )
```

```python
import jax
import jax.numpy as jnp
from jax import lax
from jax.experimental import pallas as pl
from jax.experimental.pallas import tpu as pltpu
from jax.sharding import Mesh
from jax.sharding import PartitionSpec as P

BLOCK = 128
TOPK = 16
SLOTS = 64
DESTS = 128
AREA = 66
FLAT = DESTS * AREA
PIECES = 4
PER = 8
TILES = 2
FETCH = 2
BF = jnp.bfloat16
F32 = jnp.float32
I32 = jnp.int32
NT = (((1,), (1,)), ((), ()))
VMEM = pl.BlockSpec(memory_space=pltpu.VMEM)
SMEM = pl.BlockSpec(memory_space=pltpu.SMEM)
HBM = pl.BlockSpec(memory_space=pltpu.HBM)


def group_code(g):
    high = ((g >> 11) << 3) + (((g >> 5) & 1) << 2) + ((g >> 9) & 3)
    return high, (((g >> 6) & 7) << 5) + (g & 31)


def pack_kernel(
    bounds_hbm, lengths_hbm, measures_hbm, preds_hbm, dest_hbm, keys_hbm, groups_hbm, out_hbm,
    bounds_ref, lengths_ref, measures_ref, preds_ref, dest_ref, keys_ref, groups_ref,
    area_ref, area16_ref, names_ref, values_ref, place_ref, place_smem, sems,
):
    rows = measures_ref.shape[0]
    wide = 2 * BLOCK
    sources = (preds_hbm, dest_hbm, keys_hbm, groups_hbm, bounds_hbm, lengths_hbm, measures_hbm)
    targets = (preds_ref, dest_ref, keys_ref, groups_ref, bounds_ref, lengths_ref, measures_ref)
    loads = [
        pltpu.make_async_copy(source, target, sems.at[n])
        for n, (source, target) in enumerate(zip(sources, targets))
    ]
    for load in loads:
        load.start()

    def clear(i, _):
        area_ref[pl.ds(pl.multiple_of(i * 64, 64), 64), :] = jnp.zeros((64, BLOCK), F32)
        return 0

    lax.fori_loop(0, FLAT // 64, clear, 0, unroll=4)
    for load in loads[:-1]:
        load.wait()
    lane = lax.broadcasted_iota(I32, (1, BLOCK), 1)
    before = (
        lax.broadcasted_iota(I32, (wide, wide), 0) < lax.broadcasted_iota(I32, (wide, wide), 1)
    ).astype(F32).astype(BF)
    count_of = jnp.concatenate([before, jnp.ones((wide, BLOCK), BF)], axis=1)
    dest_ids = lax.broadcasted_iota(I32, (DESTS, wide), 0)
    slot_ids = lax.broadcasted_iota(I32, (SLOTS, wide), 0)
    carry = jnp.zeros((DESTS, BLOCK), F32)
    blocks = rows // BLOCK
    places = []

    def pair(ref, step):
        return jnp.concatenate(
            [ref[2 * step : 2 * step + 1, :], ref[2 * step + 1 : 2 * step + 2, :]], axis=1
        )

    for step in range(rows // wide):
        at = pl.ds(step * wide, wide)
        ok = jnp.concatenate([lane < lengths_ref[2 * step], lane < lengths_ref[2 * step + 1]], axis=1)
        for c in range(preds_ref.shape[0]):
            v = preds_ref[c : c + 1, at]
            ok = ok & (v >= bounds_ref[c, 0]) & (v < bounds_ref[c, 1])
        target = jnp.where(ok, pair(dest_ref, step), -1)
        keys = pair(keys_ref, step)
        groups = pair(groups_ref, step)
        hit = dest_ids == target
        names = hit.astype(F32).astype(BF)
        counts = jnp.dot(names, count_of, preferred_element_type=F32)
        prior = counts[:, :wide] + jnp.concatenate([carry, carry], axis=1)
        slot = jnp.sum(jnp.where(hit, prior, 0.0), axis=0, keepdims=True).astype(I32)
        carry = carry + counts[:, wide:]
        place = jnp.where(ok, target * AREA + slot, FLAT)
        place_ref[2 * step : 2 * step + 1, :] = place[:, :BLOCK]
        place_ref[2 * step + 1 : 2 * step + 2, :] = place[:, BLOCK:]
        mine = slot_ids == slot
        values = [
            jnp.where(mine, part.astype(F32), 0.0).astype(BF)
            for part in (keys >> 8, keys & 255, *group_code(groups))
        ]
        names_ref[:, at] = names
        values_ref[:, at] = jnp.concatenate(values, axis=0)
        done = (step + 1) * 2
        if done % (blocks // 2) == 0:
            part = pl.ds(done - blocks // 2, blocks // 2)
            places.append(
                pltpu.make_async_copy(
                    place_ref.at[part], place_smem.at[part], sems.at[len(loads) + len(places)]
                )
            )
            places[-1].start()
    packed = lax.dot_general(names_ref[...], values_ref[...], NT, preferred_element_type=F32)
    for d in range(DESTS):
        area_ref[d * AREA + SLOTS : d * AREA + SLOTS + 1, :] = packed[d : d + 1, :BLOCK]
        area_ref[d * AREA + SLOTS + 1 : d * AREA + SLOTS + 2, :] = packed[d : d + 1, BLOCK:]
    loads[-1].wait()

    def put(b, _):
        for k in range(BLOCK // 16):
            x = measures_ref[pl.ds(pl.multiple_of(b * BLOCK + k * 16, 16), 16), :].astype(F32)
            for u in range(16):
                area_ref[pl.ds(place_smem[b, k * 16 + u], 1), :] = x[u : u + 1, :]
        return 0

    for n, copy in enumerate(places):
        copy.wait()
        lax.fori_loop(n * blocks // 2, (n + 1) * blocks // 2, put, 0)

    def give(i, _):
        at = pl.ds(pl.multiple_of(i * 64, 64), 64)
        area16_ref[at, :] = area_ref[at, :].astype(BF)
        return 0

    stores = []
    part = FLAT // PIECES
    for n in range(PIECES):
        lax.fori_loop(n * part // 64, (n + 1) * part // 64, give, 0, unroll=3)
        at = pl.ds(n * part, part)
        stores.append(pltpu.make_async_copy(area16_ref.at[at], out_hbm.at[at], sems.at[9 + n]))
        stores[-1].start()
    for store in stores:
        store.wait()


def pack(bounds, lengths, measures, preds, dest, keys, groups):
    rows = measures.shape[0]
    blocks = rows // BLOCK
    return pl.pallas_call(
        pack_kernel,
        out_shape=jax.ShapeDtypeStruct((FLAT, BLOCK), BF),
        in_specs=[HBM] * 7,
        out_specs=HBM,
        scratch_shapes=[
            pltpu.SMEM(bounds.shape, I32),
            pltpu.SMEM(lengths.shape, I32),
            pltpu.VMEM(measures.shape, BF),
            pltpu.VMEM(preds.shape, I32),
            pltpu.VMEM((blocks, BLOCK), I32),
            pltpu.VMEM((blocks, BLOCK), I32),
            pltpu.VMEM((blocks, BLOCK), I32),
            pltpu.VMEM((FLAT + 8, BLOCK), F32),
            pltpu.VMEM((FLAT, BLOCK), BF),
            pltpu.VMEM((DESTS, rows), BF),
            pltpu.VMEM((4 * SLOTS, rows), BF),
            pltpu.VMEM((blocks, BLOCK), I32),
            pltpu.SMEM((blocks, BLOCK), I32),
            pltpu.SemaphoreType.DMA((9 + PIECES,)),
        ],
        compiler_params=pltpu.CompilerParams(vmem_limit_bytes=58 << 20),
        name="pack",
    )(bounds, lengths, measures, preds, dest, keys, groups)


def add_groups(core, group_ref, pair_ref, sums_ref):
    rows_at = lax.broadcasted_iota(I32, (256, BLOCK), 0).astype(F32).astype(BF)
    one = jnp.ones((), BF)
    zero = jnp.zeros((), BF)
    first = (core * 4).astype(F32)
    for k in range(DESTS // 2 // PER):
        lows = []
        for p in range(k * PER, (k + 1) * PER):
            hi = group_ref[0, p : p + 1, :]
            lows.append((jnp.where(hi >= 8.0, hi - 8.0, hi) - first, group_ref[1, p : p + 1, :]))
        block = pair_ref[k * PER * BLOCK : (k + 1) * PER * BLOCK, :]
        for t in range(0, 4, TILES):
            tiles = []
            for u in range(t, t + TILES):
                cols = []
                for hi, lo in lows:
                    v = jnp.where(hi == float(u), lo, -1.0).astype(BF)
                    cols.append(jnp.where(rows_at == jnp.broadcast_to(v, (256, BLOCK)), one, zero))
                tiles.append(jnp.concatenate(cols, axis=1))
            part = jnp.dot(jnp.concatenate(tiles, axis=0), block, preferred_element_type=F32)
            at = pl.ds(t * 256, TILES * 256)
            if k == 0:
                sums_ref[at, :] = part
            else:
                sums_ref[at, :] = sums_ref[at, :] + part


def join_kernel(me_ref, got_ref, table_ref, other_ref, pair_ref, group_ref, sums_ref, turned_ref, aux_ref):
    blocks = DESTS // 2
    for d in range(DESTS):
        pair = got_ref[d * AREA + SLOTS : (d + 1) * AREA, :].astype(F32)
        aux_ref[:, d : d + 1, :] = pair.reshape(2, 1, BLOCK)

    def halves(n):
        a, b = aux_ref[n, :blocks, :], aux_ref[n, blocks:, :]
        return (
            jnp.concatenate([a[:, :SLOTS], b[:, :SLOTS]], axis=1),
            jnp.concatenate([a[:, SLOTS:], b[:, SLOTS:]], axis=1),
        )

    key_hi, key_lo = halves(0)
    grp_hi, grp_lo = halves(1)
    turned_ref[...] = jnp.concatenate([key_hi * 256.0 + key_lo, grp_hi], axis=0).T
    group_ref[0] = grp_hi
    group_ref[1] = grp_lo
    tab = jnp.concatenate([table_ref[:1024, :], table_ref[1024:, :]], axis=1)
    ids = lax.broadcasted_iota(I32, (BLOCK, 256), 1).astype(F32).astype(BF)
    one = jnp.ones((), BF)
    zero = jnp.zeros((), BF)
    for q in range(0, blocks, FETCH):
        picks = []
        uppers = []
        for p in range(q, q + FETCH):
            key = jnp.broadcast_to(turned_ref[:, p : p + 1], (BLOCK, BLOCK))
            upper = key >= 1024.0
            uppers.append(upper)
            key = jnp.where(upper, key - 1024.0, key)
            cols = []
            for t in range(4):
                k = (key - 256.0 * t).astype(BF)
                k = jnp.concatenate([k, k], axis=1)
                cols.append(jnp.where(ids == k, one, zero))
            picks.append(jnp.concatenate(cols, axis=1))
        found = jnp.dot(jnp.concatenate(picks, axis=0), tab, preferred_element_type=F32)
        for p in range(q, q + FETCH):
            mine = found[(p - q) * BLOCK : (p - q + 1) * BLOCK, :]
            row = jnp.where(uppers[p - q], mine[:, BLOCK:], mine[:, :BLOCK])
            low, high_at = p * AREA, (blocks + p) * AREA
            pay = jnp.concatenate(
                [got_ref[low : low + SLOTS, :], got_ref[high_at : high_at + SLOTS, :]], axis=0
            )
            joined = pay.astype(F32) * row
            high = jnp.broadcast_to(turned_ref[:, blocks + p : blocks + p + 1], (BLOCK, BLOCK)) >= 8.0
            none = jnp.zeros_like(joined)
            to = slice(p * BLOCK, (p + 1) * BLOCK)
            pair_ref[to, :BLOCK] = jnp.where(high, none, joined).astype(BF)
            pair_ref[to, BLOCK:] = jnp.where(high, joined, none).astype(BF)
    add_groups(1 - me_ref[0], group_ref, pair_ref, sums_ref)
    for q in range(64):
        at = slice(q % 32 * 32, (q % 32 + 1) * 32)
        other_ref[q] = sums_ref[at, q // 32 * BLOCK : (q // 32 + 1) * BLOCK].astype(BF)


def join(me, got, table):
    blocks = DESTS // 2
    return pl.pallas_call(
        join_kernel,
        out_shape=(
            jax.ShapeDtypeStruct((64, 32, BLOCK), BF),
            jax.ShapeDtypeStruct((blocks * BLOCK, 2 * BLOCK), BF),
            jax.ShapeDtypeStruct((2, blocks, BLOCK), F32),
        ),
        in_specs=[SMEM, VMEM, VMEM],
        out_specs=(VMEM, VMEM, VMEM),
        scratch_shapes=[
            pltpu.VMEM((1024, 2 * BLOCK), F32),
            pltpu.VMEM((BLOCK, BLOCK), F32),
            pltpu.VMEM((2, DESTS, BLOCK), F32),
        ],
        cost_estimate=pl.CostEstimate(flops=9 << 30, bytes_accessed=8 << 20, transcendentals=0),
        compiler_params=pltpu.CompilerParams(vmem_limit_bytes=30 << 20),
        name="join",
    )(me, got, table)


def rest_kernel(me_ref, pair_ref, group_ref, own_ref, sums_ref):
    add_groups(me_ref[0], group_ref, pair_ref, sums_ref)
    for q in range(64):
        at = slice(q % 32 * 32, (q % 32 + 1) * 32)
        own_ref[q] = sums_ref[at, q // 32 * BLOCK : (q // 32 + 1) * BLOCK]


def rest(me, pair, group):
    return pl.pallas_call(
        rest_kernel,
        out_shape=jax.ShapeDtypeStruct((64, 32, BLOCK), F32),
        in_specs=[SMEM, VMEM, VMEM],
        out_specs=VMEM,
        scratch_shapes=[pltpu.VMEM((1024, 2 * BLOCK), F32)],
        cost_estimate=pl.CostEstimate(flops=5 << 30, bytes_accessed=8 << 20, transcendentals=0),
        compiler_params=pltpu.CompilerParams(vmem_limit_bytes=24 << 20),
        name="rest",
    )(me, pair, group)


def merge_kernel(own_ref, got_ref, out_ref):
    chips, rows, _ = own_ref.shape
    total = (own_ref[...] + got_ref[...].astype(F32)).astype(BF)
    out_ref[:, :rows, :] = total
    ones = jnp.ones((8, BLOCK), BF)
    flat = total.reshape(chips * rows, BLOCK)
    means = lax.dot_general(ones, flat, NT, preferred_element_type=F32)
    score = jnp.concatenate(
        [means[0:1, n * BLOCK : (n + 1) * BLOCK] for n in range(chips * rows // BLOCK)], axis=0
    )
    score = (score * (1.0 / BLOCK)).astype(BF)
    out_ref[:, rows:, :] = jnp.broadcast_to(score[None], (chips, *score.shape))


def merge(own, got):
    chips, rows, _ = own.shape
    return pl.pallas_call(
        merge_kernel,
        out_shape=jax.ShapeDtypeStruct((chips, rows + chips * rows // BLOCK, BLOCK), BF),
        in_specs=[VMEM, VMEM],
        out_specs=VMEM,
        compiler_params=pltpu.CompilerParams(vmem_limit_bytes=16 << 20),
        name="merge",
    )(own, got)


def total_kernel(got_ref, sums_ref, score_ref):
    rows = sums_ref.shape[0]
    total = got_ref[0].astype(F32)
    for p in range(1, got_ref.shape[0]):
        total = total + got_ref[p].astype(F32)
    sums_ref[...] = total[:rows, :]
    score_ref[...] = total[rows:, :]


def total(got, rows):
    return pl.pallas_call(
        total_kernel,
        out_shape=(
            jax.ShapeDtypeStruct((rows, BLOCK), F32),
            jax.ShapeDtypeStruct((got.shape[1] - rows, BLOCK), F32),
        ),
        in_specs=[VMEM],
        out_specs=(VMEM, VMEM),
        compiler_params=pltpu.CompilerParams(vmem_limit_bytes=8 << 20),
        name="total",
    )(got)


def leaders_kernel(sums_ref, a_ref, b_ref, sums_hbm, out_ref, sem):
    copy = pltpu.make_async_copy(sums_ref, sums_hbm, sem)
    copy.start()
    x = jnp.concatenate([a_ref[...], b_ref[...]], axis=0)
    lane = lax.broadcasted_iota(I32, (1, BLOCK), 1)
    taken = jnp.zeros((1, 1), F32)
    out = jnp.full((1, BLOCK), -jnp.inf, F32)
    place = lane.astype(F32)
    for _ in range(TOPK):
        best = jnp.max(jnp.max(x, axis=0, keepdims=True), axis=1, keepdims=True)
        same = x == best
        count = jnp.sum(
            jnp.sum(same.astype(F32), axis=0, keepdims=True), axis=1, keepdims=True
        )
        out = jnp.where((place >= taken) & (place < taken + count), best, out)
        taken = taken + count
        x = jnp.where(same, -jnp.inf, x)
    out_ref[...] = out[:, :TOPK]
    copy.wait()


def leaders(sums, a, b):
    return pl.pallas_call(
        leaders_kernel,
        out_shape=(
            jax.ShapeDtypeStruct(sums.shape, F32),
            jax.ShapeDtypeStruct((1, TOPK), F32),
        ),
        in_specs=[VMEM, VMEM, VMEM],
        out_specs=(HBM, VMEM),
        scratch_shapes=[pltpu.SemaphoreType.DMA],
        compiler_params=pltpu.CompilerParams(vmem_limit_bytes=4 << 20),
        name="leaders",
    )(sums, a, b)


CHIPS = ("section", "dom_0", "dom_1")
CORE = "dom_2"
DEVICES = (*CHIPS, CORE)
SWAP = [(0, 1), (1, 0)]


def on_device(
    measures, pred_columns, bounds, lengths, destination, key_offset, group_ids, build_table
):
    blocks = measures.shape[0] // BLOCK
    me = lax.axis_index(CORE).astype(I32).reshape(1)

    def lanes(v):
        return v.reshape(blocks, BLOCK)

    me, bounds = lax.optimization_barrier((me, bounds))
    packets = pack(
        bounds, lengths, measures, pred_columns, lanes(destination), lanes(key_offset), lanes(group_ids)
    )
    got = lax.all_to_all(
        packets.reshape(DESTS, AREA // 2, 2, BLOCK), DEVICES, split_axis=0, concat_axis=0, tiled=True
    ).reshape(FLAT, BLOCK)
    theirs, joined, codes = join(me, got, build_table)
    from_partner = lax.ppermute(theirs, CORE, SWAP)
    pair = merge(rest(me, joined, codes), from_partner)
    arrived = lax.all_to_all(pair, CHIPS, split_axis=0, concat_axis=0, tiled=True)
    group_sums, scores = total(arrived, 32)
    group_sums, top = leaders(group_sums, scores, lax.ppermute(scores, CORE, SWAP))
    return group_sums, top.reshape(TOPK)


def solution(mesh):
    finer = Mesh(mesh.devices.reshape(mesh.shape["section"], 4, 4, 2), DEVICES)
    return jax.shard_map(
        on_device,
        mesh=finer,
        in_specs=(
            P(DEVICES, None),
            P(None, DEVICES),
            P(),
            P(DEVICES),
            P(DEVICES, None),
            P(DEVICES),
            P(DEVICES),
            P(DEVICES, None),
        ),
        out_specs=(P(DEVICES, None), P()),
        check_vma=False,
    )
```

```python
import jax
import jax.numpy as jnp
from jax import lax
from jax.experimental import pallas as pl
from jax.experimental.pallas import tpu as pltpu
from jax.sharding import Mesh
from jax.sharding import PartitionSpec as P

BLOCK = 128
TOPK = 16
SLOTS = 64
DESTS = 128
AREA = 66
FLAT = DESTS * AREA
PIECES = 4
PER = 8
TILES = 2
FETCH = 2
BF = jnp.bfloat16
F32 = jnp.float32
I32 = jnp.int32
NT = (((1,), (1,)), ((), ()))
VMEM = pl.BlockSpec(memory_space=pltpu.VMEM)
SMEM = pl.BlockSpec(memory_space=pltpu.SMEM)
HBM = pl.BlockSpec(memory_space=pltpu.HBM)


def group_code(g):
    high = ((g >> 11) << 3) + (((g >> 5) & 1) << 2) + ((g >> 9) & 3)
    return high, (((g >> 6) & 7) << 5) + (g & 31)


def pack_kernel(
    bounds_hbm, lengths_hbm, measures_hbm, preds_hbm, dest_hbm, keys_hbm, groups_hbm, out_hbm,
    bounds_ref, lengths_ref, measures_ref, preds_ref, dest_ref, keys_ref, groups_ref,
    area_ref, area16_ref, names_ref, values_ref, place_ref, place_smem, sems,
):
    rows = measures_ref.shape[0]
    wide = 2 * BLOCK
    sources = (preds_hbm, dest_hbm, keys_hbm, groups_hbm, bounds_hbm, lengths_hbm, measures_hbm)
    targets = (preds_ref, dest_ref, keys_ref, groups_ref, bounds_ref, lengths_ref, measures_ref)
    loads = [
        pltpu.make_async_copy(source, target, sems.at[n])
        for n, (source, target) in enumerate(zip(sources, targets))
    ]
    for load in loads:
        load.start()

    def clear(i, _):
        area_ref[pl.ds(pl.multiple_of(i * 64, 64), 64), :] = jnp.zeros((64, BLOCK), F32)
        return 0

    lax.fori_loop(0, FLAT // 64, clear, 0, unroll=4)
    for load in loads[:-1]:
        load.wait()
    lane = lax.broadcasted_iota(I32, (1, BLOCK), 1)
    before = (
        lax.broadcasted_iota(I32, (wide, wide), 0) < lax.broadcasted_iota(I32, (wide, wide), 1)
    ).astype(F32).astype(BF)
    count_of = jnp.concatenate([before, jnp.ones((wide, BLOCK), BF)], axis=1)
    dest_ids = lax.broadcasted_iota(I32, (DESTS, wide), 0)
    slot_ids = lax.broadcasted_iota(I32, (SLOTS, wide), 0)
    carry = jnp.zeros((DESTS, BLOCK), F32)
    blocks = rows // BLOCK
    places = []

    def pair(ref, step):
        return jnp.concatenate(
            [ref[2 * step : 2 * step + 1, :], ref[2 * step + 1 : 2 * step + 2, :]], axis=1
        )

    for step in range(rows // wide):
        at = pl.ds(step * wide, wide)
        ok = jnp.concatenate([lane < lengths_ref[2 * step], lane < lengths_ref[2 * step + 1]], axis=1)
        for c in range(preds_ref.shape[0]):
            v = preds_ref[c : c + 1, at]
            ok = ok & (v >= bounds_ref[c, 0]) & (v < bounds_ref[c, 1])
        target = jnp.where(ok, pair(dest_ref, step), -1)
        keys = pair(keys_ref, step)
        groups = pair(groups_ref, step)
        hit = dest_ids == target
        names = hit.astype(F32).astype(BF)
        counts = jnp.dot(names, count_of, preferred_element_type=F32)
        prior = counts[:, :wide] + jnp.concatenate([carry, carry], axis=1)
        slot = jnp.sum(jnp.where(hit, prior, 0.0), axis=0, keepdims=True).astype(I32)
        carry = carry + counts[:, wide:]
        place = jnp.where(ok, target * AREA + slot, FLAT)
        place_ref[2 * step : 2 * step + 1, :] = place[:, :BLOCK]
        place_ref[2 * step + 1 : 2 * step + 2, :] = place[:, BLOCK:]
        mine = slot_ids == slot
        values = [
            jnp.where(mine, part.astype(F32), 0.0).astype(BF)
            for part in (keys >> 8, keys & 255, *group_code(groups))
        ]
        names_ref[:, at] = names
        values_ref[:, at] = jnp.concatenate(values, axis=0)
        done = (step + 1) * 2
        if done % (blocks // 2) == 0:
            part = pl.ds(done - blocks // 2, blocks // 2)
            places.append(
                pltpu.make_async_copy(
                    place_ref.at[part], place_smem.at[part], sems.at[len(loads) + len(places)]
                )
            )
            places[-1].start()
    packed = lax.dot_general(names_ref[...], values_ref[...], NT, preferred_element_type=F32)
    for d in range(DESTS):
        area_ref[d * AREA + SLOTS : d * AREA + SLOTS + 1, :] = packed[d : d + 1, :BLOCK]
        area_ref[d * AREA + SLOTS + 1 : d * AREA + SLOTS + 2, :] = packed[d : d + 1, BLOCK:]
    loads[-1].wait()

    for n, copy in enumerate(places):
        copy.wait()
        for b in range(n * blocks // 2, (n + 1) * blocks // 2):
            for k in range(BLOCK // 16):
                first = b * BLOCK + k * 16
                x = measures_ref[first : first + 16, :].astype(F32)
                for u in range(16):
                    area_ref[pl.ds(place_smem[b, k * 16 + u], 1), :] = x[u : u + 1, :]

    def give(i, _):
        at = pl.ds(pl.multiple_of(i * 64, 64), 64)
        area16_ref[at, :] = area_ref[at, :].astype(BF)
        return 0

    stores = []
    part = FLAT // PIECES
    for n in range(PIECES):
        lax.fori_loop(n * part // 64, (n + 1) * part // 64, give, 0, unroll=3)
        at = pl.ds(n * part, part)
        stores.append(pltpu.make_async_copy(area16_ref.at[at], out_hbm.at[at], sems.at[9 + n]))
        stores[-1].start()
    for store in stores:
        store.wait()


def pack(bounds, lengths, measures, preds, dest, keys, groups):
    rows = measures.shape[0]
    blocks = rows // BLOCK
    return pl.pallas_call(
        pack_kernel,
        out_shape=jax.ShapeDtypeStruct((FLAT, BLOCK), BF),
        in_specs=[HBM] * 7,
        out_specs=HBM,
        scratch_shapes=[
            pltpu.SMEM(bounds.shape, I32),
            pltpu.SMEM(lengths.shape, I32),
            pltpu.VMEM(measures.shape, BF),
            pltpu.VMEM(preds.shape, I32),
            pltpu.VMEM((blocks, BLOCK), I32),
            pltpu.VMEM((blocks, BLOCK), I32),
            pltpu.VMEM((blocks, BLOCK), I32),
            pltpu.VMEM((FLAT + 8, BLOCK), F32),
            pltpu.VMEM((FLAT, BLOCK), BF),
            pltpu.VMEM((DESTS, rows), BF),
            pltpu.VMEM((4 * SLOTS, rows), BF),
            pltpu.VMEM((blocks, BLOCK), I32),
            pltpu.SMEM((blocks, BLOCK), I32),
            pltpu.SemaphoreType.DMA((9 + PIECES,)),
        ],
        compiler_params=pltpu.CompilerParams(vmem_limit_bytes=58 << 20),
        name="pack",
    )(bounds, lengths, measures, preds, dest, keys, groups)


def add_groups(core, group_ref, pair_ref, sums_ref):
    rows_at = lax.broadcasted_iota(I32, (256, BLOCK), 0).astype(F32).astype(BF)
    one = jnp.ones((), BF)
    zero = jnp.zeros((), BF)
    first = (core * 4).astype(F32)
    for k in range(DESTS // 2 // PER):
        lows = []
        for p in range(k * PER, (k + 1) * PER):
            hi = group_ref[0, p : p + 1, :]
            lows.append((jnp.where(hi >= 8.0, hi - 8.0, hi) - first, group_ref[1, p : p + 1, :]))
        block = pair_ref[k * PER * BLOCK : (k + 1) * PER * BLOCK, :]
        for t in range(0, 4, TILES):
            tiles = []
            for u in range(t, t + TILES):
                cols = []
                for hi, lo in lows:
                    v = jnp.where(hi == float(u), lo, -1.0).astype(BF)
                    cols.append(jnp.where(rows_at == jnp.broadcast_to(v, (256, BLOCK)), one, zero))
                tiles.append(jnp.concatenate(cols, axis=1))
            part = jnp.dot(jnp.concatenate(tiles, axis=0), block, preferred_element_type=F32)
            at = pl.ds(t * 256, TILES * 256)
            if k == 0:
                sums_ref[at, :] = part
            else:
                sums_ref[at, :] = sums_ref[at, :] + part


def join_kernel(me_ref, got_ref, table_ref, other_ref, pair_ref, group_ref, sums_ref, turned_ref, aux_ref):
    blocks = DESTS // 2
    for d in range(DESTS):
        pair = got_ref[d * AREA + SLOTS : (d + 1) * AREA, :].astype(F32)
        aux_ref[:, d : d + 1, :] = pair.reshape(2, 1, BLOCK)

    def halves(n):
        a, b = aux_ref[n, :blocks, :], aux_ref[n, blocks:, :]
        return (
            jnp.concatenate([a[:, :SLOTS], b[:, :SLOTS]], axis=1),
            jnp.concatenate([a[:, SLOTS:], b[:, SLOTS:]], axis=1),
        )

    key_hi, key_lo = halves(0)
    grp_hi, grp_lo = halves(1)
    turned_ref[...] = jnp.concatenate([key_hi * 256.0 + key_lo, grp_hi], axis=0).T
    group_ref[0] = grp_hi
    group_ref[1] = grp_lo
    tab = jnp.concatenate([table_ref[:1024, :], table_ref[1024:, :]], axis=1)
    ids = lax.broadcasted_iota(I32, (BLOCK, 256), 1).astype(F32).astype(BF)
    one = jnp.ones((), BF)
    zero = jnp.zeros((), BF)
    for q in range(0, blocks, FETCH):
        picks = []
        uppers = []
        for p in range(q, q + FETCH):
            key = jnp.broadcast_to(turned_ref[:, p : p + 1], (BLOCK, BLOCK))
            upper = key >= 1024.0
            uppers.append(upper)
            key = jnp.where(upper, key - 1024.0, key)
            cols = []
            for t in range(4):
                k = (key - 256.0 * t).astype(BF)
                k = jnp.concatenate([k, k], axis=1)
                cols.append(jnp.where(ids == k, one, zero))
            picks.append(jnp.concatenate(cols, axis=1))
        found = jnp.dot(jnp.concatenate(picks, axis=0), tab, preferred_element_type=F32)
        for p in range(q, q + FETCH):
            mine = found[(p - q) * BLOCK : (p - q + 1) * BLOCK, :]
            row = jnp.where(uppers[p - q], mine[:, BLOCK:], mine[:, :BLOCK])
            low, high_at = p * AREA, (blocks + p) * AREA
            pay = jnp.concatenate(
                [got_ref[low : low + SLOTS, :], got_ref[high_at : high_at + SLOTS, :]], axis=0
            )
            joined = pay.astype(F32) * row
            high = jnp.broadcast_to(turned_ref[:, blocks + p : blocks + p + 1], (BLOCK, BLOCK)) >= 8.0
            none = jnp.zeros_like(joined)
            to = slice(p * BLOCK, (p + 1) * BLOCK)
            pair_ref[to, :BLOCK] = jnp.where(high, none, joined).astype(BF)
            pair_ref[to, BLOCK:] = jnp.where(high, joined, none).astype(BF)
    add_groups(1 - me_ref[0], group_ref, pair_ref, sums_ref)
    for q in range(64):
        at = slice(q % 32 * 32, (q % 32 + 1) * 32)
        other_ref[q] = sums_ref[at, q // 32 * BLOCK : (q // 32 + 1) * BLOCK].astype(BF)


def join(me, got, table):
    blocks = DESTS // 2
    return pl.pallas_call(
        join_kernel,
        out_shape=(
            jax.ShapeDtypeStruct((64, 32, BLOCK), BF),
            jax.ShapeDtypeStruct((blocks * BLOCK, 2 * BLOCK), BF),
            jax.ShapeDtypeStruct((2, blocks, BLOCK), F32),
        ),
        in_specs=[SMEM, VMEM, VMEM],
        out_specs=(VMEM, VMEM, VMEM),
        scratch_shapes=[
            pltpu.VMEM((1024, 2 * BLOCK), F32),
            pltpu.VMEM((BLOCK, BLOCK), F32),
            pltpu.VMEM((2, DESTS, BLOCK), F32),
        ],
        cost_estimate=pl.CostEstimate(flops=9 << 30, bytes_accessed=8 << 20, transcendentals=0),
        compiler_params=pltpu.CompilerParams(vmem_limit_bytes=30 << 20),
        name="join",
    )(me, got, table)


def rest_kernel(me_ref, pair_ref, group_ref, own_ref, sums_ref):
    add_groups(me_ref[0], group_ref, pair_ref, sums_ref)
    for q in range(64):
        at = slice(q % 32 * 32, (q % 32 + 1) * 32)
        own_ref[q] = sums_ref[at, q // 32 * BLOCK : (q // 32 + 1) * BLOCK]


def rest(me, pair, group):
    return pl.pallas_call(
        rest_kernel,
        out_shape=jax.ShapeDtypeStruct((64, 32, BLOCK), F32),
        in_specs=[SMEM, VMEM, VMEM],
        out_specs=VMEM,
        scratch_shapes=[pltpu.VMEM((1024, 2 * BLOCK), F32)],
        cost_estimate=pl.CostEstimate(flops=5 << 30, bytes_accessed=8 << 20, transcendentals=0),
        compiler_params=pltpu.CompilerParams(vmem_limit_bytes=24 << 20),
        name="rest",
    )(me, pair, group)


def merge_kernel(own_ref, got_ref, out_ref):
    chips, rows, _ = own_ref.shape
    total = (own_ref[...] + got_ref[...].astype(F32)).astype(BF)
    out_ref[:, :rows, :] = total
    ones = jnp.ones((8, BLOCK), BF)
    flat = total.reshape(chips * rows, BLOCK)
    means = lax.dot_general(ones, flat, NT, preferred_element_type=F32)
    score = jnp.concatenate(
        [means[0:1, n * BLOCK : (n + 1) * BLOCK] for n in range(chips * rows // BLOCK)], axis=0
    )
    score = (score * (1.0 / BLOCK)).astype(BF)
    out_ref[:, rows:, :] = jnp.broadcast_to(score[None], (chips, *score.shape))


def merge(own, got):
    chips, rows, _ = own.shape
    return pl.pallas_call(
        merge_kernel,
        out_shape=jax.ShapeDtypeStruct((chips, rows + chips * rows // BLOCK, BLOCK), BF),
        in_specs=[VMEM, VMEM],
        out_specs=VMEM,
        compiler_params=pltpu.CompilerParams(vmem_limit_bytes=16 << 20),
        name="merge",
    )(own, got)


def total_kernel(got_ref, sums_ref, score_ref):
    rows = sums_ref.shape[0]
    total = got_ref[0].astype(F32)
    for p in range(1, got_ref.shape[0]):
        total = total + got_ref[p].astype(F32)
    sums_ref[...] = total[:rows, :]
    score_ref[...] = total[rows:, :]


def total(got, rows):
    return pl.pallas_call(
        total_kernel,
        out_shape=(
            jax.ShapeDtypeStruct((rows, BLOCK), F32),
            jax.ShapeDtypeStruct((got.shape[1] - rows, BLOCK), F32),
        ),
        in_specs=[VMEM],
        out_specs=(VMEM, VMEM),
        compiler_params=pltpu.CompilerParams(vmem_limit_bytes=8 << 20),
        name="total",
    )(got)


def leaders_kernel(sums_ref, a_ref, b_ref, sums_hbm, out_ref, sem):
    copy = pltpu.make_async_copy(sums_ref, sums_hbm, sem)
    copy.start()
    x = jnp.concatenate([a_ref[...], b_ref[...]], axis=0)
    lanes = 4 * BLOCK

    def ids(shape, dim):
        return lax.broadcasted_iota(I32, shape, dim)

    def column(v):
        return jnp.broadcast_to(v, (BLOCK, BLOCK)).T

    best = jnp.max(x, axis=0, keepdims=True)
    down = column(best)
    square = (BLOCK, BLOCK)
    over = (down > best) | ((down == best) & (ids(square, 0) < ids(square, 1)))
    rank = jnp.sum(over.astype(F32), axis=0, keepdims=True).astype(I32)
    pick = (ids((TOPK, BLOCK), 0) == rank).astype(F32)
    found = lax.dot_general(
        pick, x, NT, precision=lax.Precision.HIGHEST, preferred_element_type=F32
    )
    spread = (ids((x.shape[0], lanes), 0) == ids((x.shape[0], lanes), 1) % x.shape[0]).astype(F32)
    tiled = jnp.dot(found, spread, precision=lax.Precision.HIGHEST, preferred_element_type=F32)
    keep = ids((TOPK, lanes), 0) == ids((TOPK, lanes), 1) // x.shape[0]
    flat = jnp.sum(jnp.where(keep, tiled, 0.0), axis=0, keepdims=True)
    pieces = [flat[:, n * BLOCK : (n + 1) * BLOCK] for n in range(4)]
    out = jnp.zeros((1, BLOCK), F32)
    for m in range(4):
        down = column(pieces[m])
        wins = jnp.zeros(square, F32)
        for n in range(4):
            over = pieces[n] > down
            if n < m:
                over = over | (pieces[n] == down)
            elif n == m:
                over = over | ((pieces[n] == down) & (ids(square, 1) < ids(square, 0)))
            wins = wins + over.astype(F32)
        place = jnp.sum(wins, axis=1, keepdims=True).astype(I32)
        out = out + jnp.sum(jnp.where(place == ids(square, 1), down, 0.0), axis=0, keepdims=True)
    out_ref[...] = out[:, :TOPK]
    copy.wait()


def leaders(sums, a, b):
    return pl.pallas_call(
        leaders_kernel,
        out_shape=(
            jax.ShapeDtypeStruct(sums.shape, F32),
            jax.ShapeDtypeStruct((1, TOPK), F32),
        ),
        in_specs=[VMEM, VMEM, VMEM],
        out_specs=(HBM, VMEM),
        scratch_shapes=[pltpu.SemaphoreType.DMA],
        compiler_params=pltpu.CompilerParams(vmem_limit_bytes=4 << 20),
        name="leaders",
    )(sums, a, b)


CHIPS = ("section", "dom_0", "dom_1")
CORE = "dom_2"
DEVICES = (*CHIPS, CORE)
SWAP = [(0, 1), (1, 0)]


def on_device(
    measures, pred_columns, bounds, lengths, destination, key_offset, group_ids, build_table
):
    blocks = measures.shape[0] // BLOCK
    me = lax.axis_index(CORE).astype(I32).reshape(1)

    def lanes(v):
        return v.reshape(blocks, BLOCK)

    me, bounds = lax.optimization_barrier((me, bounds))
    packets = pack(
        bounds, lengths, measures, pred_columns, lanes(destination), lanes(key_offset), lanes(group_ids)
    )
    got = lax.all_to_all(
        packets.reshape(DESTS, AREA // 2, 2, BLOCK), DEVICES, split_axis=0, concat_axis=0, tiled=True
    ).reshape(FLAT, BLOCK)
    theirs, joined, codes = join(me, got, build_table)
    from_partner = lax.ppermute(theirs, CORE, SWAP)
    pair = merge(rest(me, joined, codes), from_partner)
    arrived = lax.all_to_all(pair, CHIPS, split_axis=0, concat_axis=0, tiled=True)
    group_sums, scores = total(arrived, 32)
    group_sums, top = leaders(group_sums, scores, lax.ppermute(scores, CORE, SWAP))
    return group_sums, top.reshape(TOPK)


def solution(mesh):
    finer = Mesh(mesh.devices.reshape(mesh.shape["section"], 4, 4, 2), DEVICES)
    return jax.shard_map(
        on_device,
        mesh=finer,
        in_specs=(
            P(DEVICES, None),
            P(None, DEVICES),
            P(),
            P(DEVICES),
            P(DEVICES, None),
            P(DEVICES),
            P(DEVICES),
            P(DEVICES, None),
        ),
        out_specs=(P(DEVICES, None), P()),
        check_vma=False,
    )
```

```python
import jax
import jax.numpy as jnp
from jax import lax
from jax.experimental import pallas as pl
from jax.experimental.pallas import tpu as pltpu
from jax.sharding import Mesh
from jax.sharding import PartitionSpec as P

BLOCK = 128
TOPK = 16
SLOTS = 64
DESTS = 128
AREA = 66
FLAT = DESTS * AREA
PIECES = 4
PER = 8
TILES = 2
FETCH = 2
BF = jnp.bfloat16
F32 = jnp.float32
I32 = jnp.int32
NT = (((1,), (1,)), ((), ()))
VMEM = pl.BlockSpec(memory_space=pltpu.VMEM)
SMEM = pl.BlockSpec(memory_space=pltpu.SMEM)
HBM = pl.BlockSpec(memory_space=pltpu.HBM)


def group_code(g):
    high = ((g >> 11) << 3) + (((g >> 5) & 1) << 2) + ((g >> 9) & 3)
    return high, (((g >> 6) & 7) << 5) + (g & 31)


def pack_kernel(
    bounds_hbm, lengths_hbm, measures_hbm, preds_hbm, dest_hbm, keys_hbm, groups_hbm, out_hbm,
    bounds_ref, lengths_ref, measures_ref, preds_ref, dest_ref, keys_ref, groups_ref,
    area_ref, area16_ref, names_ref, values_ref, place_ref, place_smem, sems,
):
    rows = measures_ref.shape[0]
    wide = 2 * BLOCK
    sources = (preds_hbm, dest_hbm, keys_hbm, groups_hbm, bounds_hbm, lengths_hbm, measures_hbm)
    targets = (preds_ref, dest_ref, keys_ref, groups_ref, bounds_ref, lengths_ref, measures_ref)
    loads = [
        pltpu.make_async_copy(source, target, sems.at[n])
        for n, (source, target) in enumerate(zip(sources, targets))
    ]
    for load in loads:
        load.start()

    def clear(i, _):
        area_ref[pl.ds(pl.multiple_of(i * 64, 64), 64), :] = jnp.zeros((64, BLOCK), F32)
        return 0

    lax.fori_loop(0, FLAT // 64, clear, 0, unroll=4)
    for load in loads[:-1]:
        load.wait()
    lane = lax.broadcasted_iota(I32, (1, BLOCK), 1)
    before = (
        lax.broadcasted_iota(I32, (wide, wide), 0) < lax.broadcasted_iota(I32, (wide, wide), 1)
    ).astype(F32).astype(BF)
    count_of = jnp.concatenate([before, jnp.ones((wide, BLOCK), BF)], axis=1)
    dest_ids = lax.broadcasted_iota(I32, (DESTS, wide), 0)
    slot_ids = lax.broadcasted_iota(I32, (SLOTS, wide), 0)
    carry = jnp.zeros((DESTS, BLOCK), F32)
    blocks = rows // BLOCK
    places = []

    def pair(ref, step):
        return jnp.concatenate(
            [ref[2 * step : 2 * step + 1, :], ref[2 * step + 1 : 2 * step + 2, :]], axis=1
        )

    for step in range(rows // wide):
        at = pl.ds(step * wide, wide)
        ok = jnp.concatenate([lane < lengths_ref[2 * step], lane < lengths_ref[2 * step + 1]], axis=1)
        for c in range(preds_ref.shape[0]):
            v = preds_ref[c : c + 1, at]
            ok = ok & (v >= bounds_ref[c, 0]) & (v < bounds_ref[c, 1])
        target = jnp.where(ok, pair(dest_ref, step), -1)
        keys = pair(keys_ref, step)
        groups = pair(groups_ref, step)
        hit = dest_ids == target
        names = hit.astype(F32).astype(BF)
        counts = jnp.dot(names, count_of, preferred_element_type=F32)
        prior = counts[:, :wide] + jnp.concatenate([carry, carry], axis=1)
        slot = jnp.sum(jnp.where(hit, prior, 0.0), axis=0, keepdims=True).astype(I32)
        carry = carry + counts[:, wide:]
        place = jnp.where(ok, target * AREA + slot, FLAT)
        place_ref[2 * step : 2 * step + 1, :] = place[:, :BLOCK]
        place_ref[2 * step + 1 : 2 * step + 2, :] = place[:, BLOCK:]
        mine = slot_ids == slot
        values = [
            jnp.where(mine, part.astype(F32), 0.0).astype(BF)
            for part in (keys >> 8, keys & 255, *group_code(groups))
        ]
        names_ref[:, at] = names
        values_ref[:, at] = jnp.concatenate(values, axis=0)
        done = (step + 1) * 2
        if done % (blocks // 2) == 0:
            part = pl.ds(done - blocks // 2, blocks // 2)
            places.append(
                pltpu.make_async_copy(
                    place_ref.at[part], place_smem.at[part], sems.at[len(loads) + len(places)]
                )
            )
            places[-1].start()
    packed = lax.dot_general(names_ref[...], values_ref[...], NT, preferred_element_type=F32)
    for d in range(DESTS):
        area_ref[d * AREA + SLOTS : d * AREA + SLOTS + 1, :] = packed[d : d + 1, :BLOCK]
        area_ref[d * AREA + SLOTS + 1 : d * AREA + SLOTS + 2, :] = packed[d : d + 1, BLOCK:]
    loads[-1].wait()

    for n, copy in enumerate(places):
        copy.wait()
        for b in range(n * blocks // 2, (n + 1) * blocks // 2):
            for k in range(BLOCK // 16):
                first = b * BLOCK + k * 16
                x = measures_ref[first : first + 16, :].astype(F32)
                for u in range(16):
                    area_ref[pl.ds(place_smem[b, k * 16 + u], 1), :] = x[u : u + 1, :]

    def give(i, _):
        at = pl.ds(pl.multiple_of(i * 64, 64), 64)
        area16_ref[at, :] = area_ref[at, :].astype(BF)
        return 0

    stores = []
    part = FLAT // PIECES
    for n in range(PIECES):
        lax.fori_loop(n * part // 64, (n + 1) * part // 64, give, 0, unroll=3)
        at = pl.ds(n * part, part)
        stores.append(pltpu.make_async_copy(area16_ref.at[at], out_hbm.at[at], sems.at[9 + n]))
        stores[-1].start()
    for store in stores:
        store.wait()


def pack(bounds, lengths, measures, preds, dest, keys, groups):
    rows = measures.shape[0]
    blocks = rows // BLOCK
    return pl.pallas_call(
        pack_kernel,
        out_shape=jax.ShapeDtypeStruct((FLAT, BLOCK), BF),
        in_specs=[HBM] * 7,
        out_specs=HBM,
        scratch_shapes=[
            pltpu.SMEM(bounds.shape, I32),
            pltpu.SMEM(lengths.shape, I32),
            pltpu.VMEM(measures.shape, BF),
            pltpu.VMEM(preds.shape, I32),
            pltpu.VMEM((blocks, BLOCK), I32),
            pltpu.VMEM((blocks, BLOCK), I32),
            pltpu.VMEM((blocks, BLOCK), I32),
            pltpu.VMEM((FLAT + 8, BLOCK), F32),
            pltpu.VMEM((FLAT, BLOCK), BF),
            pltpu.VMEM((DESTS, rows), BF),
            pltpu.VMEM((4 * SLOTS, rows), BF),
            pltpu.VMEM((blocks, BLOCK), I32),
            pltpu.SMEM((blocks, BLOCK), I32),
            pltpu.SemaphoreType.DMA((9 + PIECES,)),
        ],
        compiler_params=pltpu.CompilerParams(vmem_limit_bytes=58 << 20),
        name="pack",
    )(bounds, lengths, measures, preds, dest, keys, groups)


def add_groups(core, group_ref, pair_ref, sums_ref):
    rows_at = lax.broadcasted_iota(I32, (256, BLOCK), 0).astype(F32).astype(BF)
    one = jnp.ones((), BF)
    zero = jnp.zeros((), BF)
    first = (core * 4).astype(F32)
    for k in range(DESTS // 2 // PER):
        lows = []
        for p in range(k * PER, (k + 1) * PER):
            hi = group_ref[0, p : p + 1, :]
            lows.append((jnp.where(hi >= 8.0, hi - 8.0, hi) - first, group_ref[1, p : p + 1, :]))
        block = pair_ref[k * PER * BLOCK : (k + 1) * PER * BLOCK, :]
        for t in range(0, 4, TILES):
            tiles = []
            for u in range(t, t + TILES):
                cols = []
                for hi, lo in lows:
                    v = jnp.where(hi == float(u), lo, -1.0).astype(BF)
                    cols.append(jnp.where(rows_at == jnp.broadcast_to(v, (256, BLOCK)), one, zero))
                tiles.append(jnp.concatenate(cols, axis=1))
            part = jnp.dot(jnp.concatenate(tiles, axis=0), block, preferred_element_type=F32)
            at = pl.ds(t * 256, TILES * 256)
            if k == 0:
                sums_ref[at, :] = part
            else:
                sums_ref[at, :] = sums_ref[at, :] + part


def join_kernel(me_ref, got_ref, table_ref, other_ref, pair_ref, group_ref, sums_ref, turned_ref, aux_ref):
    blocks = DESTS // 2
    for d in range(DESTS):
        pair = got_ref[d * AREA + SLOTS : (d + 1) * AREA, :].astype(F32)
        aux_ref[:, d : d + 1, :] = pair.reshape(2, 1, BLOCK)

    def halves(n):
        a, b = aux_ref[n, :blocks, :], aux_ref[n, blocks:, :]
        return (
            jnp.concatenate([a[:, :SLOTS], b[:, :SLOTS]], axis=1),
            jnp.concatenate([a[:, SLOTS:], b[:, SLOTS:]], axis=1),
        )

    key_hi, key_lo = halves(0)
    grp_hi, grp_lo = halves(1)
    turned_ref[...] = jnp.concatenate([key_hi * 256.0 + key_lo, grp_hi], axis=0).T
    group_ref[0] = grp_hi
    group_ref[1] = grp_lo
    tab = jnp.concatenate([table_ref[:1024, :], table_ref[1024:, :]], axis=1)
    ids = lax.broadcasted_iota(I32, (BLOCK, 256), 1).astype(F32).astype(BF)
    one = jnp.ones((), BF)
    zero = jnp.zeros((), BF)
    for q in range(0, blocks, FETCH):
        picks = []
        uppers = []
        for p in range(q, q + FETCH):
            key = jnp.broadcast_to(turned_ref[:, p : p + 1], (BLOCK, BLOCK))
            upper = key >= 1024.0
            uppers.append(upper)
            key = jnp.where(upper, key - 1024.0, key)
            cols = []
            for t in range(4):
                k = (key - 256.0 * t).astype(BF)
                k = jnp.concatenate([k, k], axis=1)
                cols.append(jnp.where(ids == k, one, zero))
            picks.append(jnp.concatenate(cols, axis=1))
        found = jnp.dot(jnp.concatenate(picks, axis=0), tab, preferred_element_type=F32)
        for p in range(q, q + FETCH):
            mine = found[(p - q) * BLOCK : (p - q + 1) * BLOCK, :]
            row = jnp.where(uppers[p - q], mine[:, BLOCK:], mine[:, :BLOCK])
            low, high_at = p * AREA, (blocks + p) * AREA
            pay = jnp.concatenate(
                [got_ref[low : low + SLOTS, :], got_ref[high_at : high_at + SLOTS, :]], axis=0
            )
            joined = pay.astype(F32) * row
            high = jnp.broadcast_to(turned_ref[:, blocks + p : blocks + p + 1], (BLOCK, BLOCK)) >= 8.0
            none = jnp.zeros_like(joined)
            to = slice(p * BLOCK, (p + 1) * BLOCK)
            pair_ref[to, :BLOCK] = jnp.where(high, none, joined).astype(BF)
            pair_ref[to, BLOCK:] = jnp.where(high, joined, none).astype(BF)
    add_groups(1 - me_ref[0], group_ref, pair_ref, sums_ref)
    for q in range(64):
        at = slice(q % 32 * 32, (q % 32 + 1) * 32)
        other_ref[q] = sums_ref[at, q // 32 * BLOCK : (q // 32 + 1) * BLOCK].astype(BF)


def join(me, got, table):
    blocks = DESTS // 2
    return pl.pallas_call(
        join_kernel,
        out_shape=(
            jax.ShapeDtypeStruct((64, 32, BLOCK), BF),
            jax.ShapeDtypeStruct((blocks * BLOCK, 2 * BLOCK), BF),
            jax.ShapeDtypeStruct((2, blocks, BLOCK), F32),
        ),
        in_specs=[SMEM, VMEM, VMEM],
        out_specs=(VMEM, VMEM, VMEM),
        scratch_shapes=[
            pltpu.VMEM((1024, 2 * BLOCK), F32),
            pltpu.VMEM((BLOCK, BLOCK), F32),
            pltpu.VMEM((2, DESTS, BLOCK), F32),
        ],
        cost_estimate=pl.CostEstimate(flops=9 << 30, bytes_accessed=8 << 20, transcendentals=0),
        compiler_params=pltpu.CompilerParams(vmem_limit_bytes=30 << 20),
        name="join",
    )(me, got, table)


def rest_kernel(me_ref, pair_ref, group_ref, own_ref, sums_ref):
    add_groups(me_ref[0], group_ref, pair_ref, sums_ref)
    for q in range(64):
        at = slice(q % 32 * 32, (q % 32 + 1) * 32)
        own_ref[q] = sums_ref[at, q // 32 * BLOCK : (q // 32 + 1) * BLOCK]


def rest(me, pair, group):
    return pl.pallas_call(
        rest_kernel,
        out_shape=jax.ShapeDtypeStruct((64, 32, BLOCK), F32),
        in_specs=[SMEM, VMEM, VMEM],
        out_specs=VMEM,
        scratch_shapes=[pltpu.VMEM((1024, 2 * BLOCK), F32)],
        cost_estimate=pl.CostEstimate(flops=5 << 30, bytes_accessed=8 << 20, transcendentals=0),
        compiler_params=pltpu.CompilerParams(vmem_limit_bytes=24 << 20),
        name="rest",
    )(me, pair, group)


def merge_kernel(own_ref, got_ref, out_ref):
    chips, rows, _ = own_ref.shape
    total = (own_ref[...] + got_ref[...].astype(F32)).astype(BF)
    out_ref[:, :rows, :] = total
    ones = jnp.ones((8, BLOCK), BF)
    flat = total.reshape(chips * rows, BLOCK)
    means = lax.dot_general(ones, flat, NT, preferred_element_type=F32)
    score = jnp.concatenate(
        [means[0:1, n * BLOCK : (n + 1) * BLOCK] for n in range(chips * rows // BLOCK)], axis=0
    )
    score = (score * (1.0 / BLOCK)).astype(BF)
    out_ref[:, rows:, :] = jnp.broadcast_to(score[None], (chips, *score.shape))


def merge(own, got):
    chips, rows, _ = own.shape
    return pl.pallas_call(
        merge_kernel,
        out_shape=jax.ShapeDtypeStruct((chips, rows + chips * rows // BLOCK, BLOCK), BF),
        in_specs=[VMEM, VMEM],
        out_specs=VMEM,
        compiler_params=pltpu.CompilerParams(vmem_limit_bytes=16 << 20),
        name="merge",
    )(own, got)


def total_kernel(got_ref, sums_ref, score_ref):
    rows = sums_ref.shape[0]
    total = got_ref[0].astype(F32)
    for p in range(1, got_ref.shape[0]):
        total = total + got_ref[p].astype(F32)
    sums_ref[...] = total[:rows, :]
    score_ref[...] = total[rows:, :]


def total(got, rows):
    return pl.pallas_call(
        total_kernel,
        out_shape=(
            jax.ShapeDtypeStruct((rows, BLOCK), F32),
            jax.ShapeDtypeStruct((got.shape[1] - rows, BLOCK), F32),
        ),
        in_specs=[VMEM],
        out_specs=(VMEM, VMEM),
        compiler_params=pltpu.CompilerParams(vmem_limit_bytes=8 << 20),
        name="total",
    )(got)


def leaders_kernel(sums_ref, a_ref, b_ref, sums_hbm, out_ref, sem):
    copy = pltpu.make_async_copy(sums_ref, sums_hbm, sem)
    copy.start()
    x = jnp.concatenate([a_ref[...], b_ref[...]], axis=0)
    lanes = 4 * BLOCK

    def ids(shape, dim):
        return lax.broadcasted_iota(I32, shape, dim)

    def column(v):
        return jnp.broadcast_to(v, (BLOCK, BLOCK)).T

    best = jnp.max(x, axis=0, keepdims=True)
    down = column(best)
    square = (BLOCK, BLOCK)
    over = (down > best) | ((down == best) & (ids(square, 0) < ids(square, 1)))
    rank = jnp.sum(over.astype(F32), axis=0, keepdims=True).astype(I32)
    pick = (ids((TOPK, BLOCK), 0) == rank).astype(F32)
    copies = jnp.concatenate([x] * TOPK, axis=0)
    tiled = lax.dot_general(
        pick, copies, NT, precision=lax.Precision.HIGHEST, preferred_element_type=F32
    )
    keep = ids((TOPK, lanes), 0) == ids((TOPK, lanes), 1) // x.shape[0]
    flat = jnp.sum(jnp.where(keep, tiled, 0.0), axis=0, keepdims=True)
    pieces = [flat[:, n * BLOCK : (n + 1) * BLOCK] for n in range(4)]
    out = jnp.zeros((1, BLOCK), F32)
    for m in range(4):
        down = column(pieces[m])
        wins = jnp.zeros(square, F32)
        for n in range(4):
            over = pieces[n] > down
            if n < m:
                over = over | (pieces[n] == down)
            elif n == m:
                over = over | ((pieces[n] == down) & (ids(square, 1) < ids(square, 0)))
            wins = wins + over.astype(F32)
        place = jnp.sum(wins, axis=1, keepdims=True).astype(I32)
        out = out + jnp.sum(jnp.where(place == ids(square, 1), down, 0.0), axis=0, keepdims=True)
    out_ref[...] = out[:, :TOPK]
    copy.wait()


def leaders(sums, a, b):
    return pl.pallas_call(
        leaders_kernel,
        out_shape=(
            jax.ShapeDtypeStruct(sums.shape, F32),
            jax.ShapeDtypeStruct((1, TOPK), F32),
        ),
        in_specs=[VMEM, VMEM, VMEM],
        out_specs=(HBM, VMEM),
        scratch_shapes=[pltpu.SemaphoreType.DMA],
        compiler_params=pltpu.CompilerParams(vmem_limit_bytes=4 << 20),
        name="leaders",
    )(sums, a, b)


CHIPS = ("section", "dom_0", "dom_1")
CORE = "dom_2"
DEVICES = (*CHIPS, CORE)
SWAP = [(0, 1), (1, 0)]


def on_device(
    measures, pred_columns, bounds, lengths, destination, key_offset, group_ids, build_table
):
    blocks = measures.shape[0] // BLOCK
    me = lax.axis_index(CORE).astype(I32).reshape(1)

    def lanes(v):
        return v.reshape(blocks, BLOCK)

    me, bounds = lax.optimization_barrier((me, bounds))
    packets = pack(
        bounds, lengths, measures, pred_columns, lanes(destination), lanes(key_offset), lanes(group_ids)
    )
    got = lax.all_to_all(
        packets.reshape(DESTS, AREA // 2, 2, BLOCK), DEVICES, split_axis=0, concat_axis=0, tiled=True
    ).reshape(FLAT, BLOCK)
    theirs, joined, codes = join(me, got, build_table)
    from_partner = lax.ppermute(theirs, CORE, SWAP)
    pair = merge(rest(me, joined, codes), from_partner)
    arrived = lax.all_to_all(pair, CHIPS, split_axis=0, concat_axis=0, tiled=True)
    group_sums, scores = total(arrived, 32)
    group_sums, top = leaders(group_sums, scores, lax.ppermute(scores, CORE, SWAP))
    return group_sums, top.reshape(TOPK)


def solution(mesh):
    finer = Mesh(mesh.devices.reshape(mesh.shape["section"], 4, 4, 2), DEVICES)
    return jax.shard_map(
        on_device,
        mesh=finer,
        in_specs=(
            P(DEVICES, None),
            P(None, DEVICES),
            P(),
            P(DEVICES),
            P(DEVICES, None),
            P(DEVICES),
            P(DEVICES),
            P(DEVICES, None),
        ),
        out_specs=(P(DEVICES, None), P()),
        check_vma=False,
    )
```

```python
import jax
import jax.numpy as jnp
from jax import lax
from jax.experimental import pallas as pl
from jax.experimental.pallas import tpu as pltpu
from jax.sharding import Mesh
from jax.sharding import PartitionSpec as P

BLOCK = 128
TOPK = 16
SLOTS = 64
DESTS = 128
AREA = 66
FLAT = DESTS * AREA
PIECES = 4
PER = 8
TILES = 4
FETCH = 4
BF = jnp.bfloat16
F32 = jnp.float32
I32 = jnp.int32
NT = (((1,), (1,)), ((), ()))
VMEM = pl.BlockSpec(memory_space=pltpu.VMEM)
SMEM = pl.BlockSpec(memory_space=pltpu.SMEM)
HBM = pl.BlockSpec(memory_space=pltpu.HBM)


def group_code(g):
    high = ((g >> 11) << 3) + (((g >> 5) & 1) << 2) + ((g >> 9) & 3)
    return high, (((g >> 6) & 7) << 5) + (g & 31)


def pack_kernel(
    bounds_hbm, lengths_hbm, measures_hbm, preds_hbm, dest_hbm, keys_hbm, groups_hbm, out_hbm,
    bounds_ref, lengths_ref, measures_ref, preds_ref, dest_ref, keys_ref, groups_ref,
    area_ref, area16_ref, names_ref, values_ref, place_ref, place_smem, sems,
):
    rows = measures_ref.shape[0]
    wide = 2 * BLOCK
    sources = (preds_hbm, dest_hbm, keys_hbm, groups_hbm, bounds_hbm, lengths_hbm, measures_hbm)
    targets = (preds_ref, dest_ref, keys_ref, groups_ref, bounds_ref, lengths_ref, measures_ref)
    loads = [
        pltpu.make_async_copy(source, target, sems.at[n])
        for n, (source, target) in enumerate(zip(sources, targets))
    ]
    for load in loads:
        load.start()

    def clear(i, _):
        area_ref[pl.ds(pl.multiple_of(i * 64, 64), 64), :] = jnp.zeros((64, BLOCK), F32)
        return 0

    lax.fori_loop(0, FLAT // 64, clear, 0, unroll=4)
    for load in loads[:-1]:
        load.wait()
    lane = lax.broadcasted_iota(I32, (1, BLOCK), 1)
    before = (
        lax.broadcasted_iota(I32, (wide, wide), 0) < lax.broadcasted_iota(I32, (wide, wide), 1)
    ).astype(F32).astype(BF)
    count_of = jnp.concatenate([before, jnp.ones((wide, BLOCK), BF)], axis=1)
    dest_ids = lax.broadcasted_iota(I32, (DESTS, wide), 0)
    slot_ids = lax.broadcasted_iota(I32, (SLOTS, wide), 0)
    carry = jnp.zeros((DESTS, BLOCK), F32)
    blocks = rows // BLOCK
    places = []

    def pair(ref, step):
        return jnp.concatenate(
            [ref[2 * step : 2 * step + 1, :], ref[2 * step + 1 : 2 * step + 2, :]], axis=1
        )

    for step in range(rows // wide):
        at = pl.ds(step * wide, wide)
        ok = jnp.concatenate([lane < lengths_ref[2 * step], lane < lengths_ref[2 * step + 1]], axis=1)
        for c in range(preds_ref.shape[0]):
            v = preds_ref[c : c + 1, at]
            ok = ok & (v >= bounds_ref[c, 0]) & (v < bounds_ref[c, 1])
        target = jnp.where(ok, pair(dest_ref, step), -1)
        keys = pair(keys_ref, step)
        groups = pair(groups_ref, step)
        hit = dest_ids == target
        names = hit.astype(F32).astype(BF)
        counts = jnp.dot(names, count_of, preferred_element_type=F32)
        prior = counts[:, :wide] + jnp.concatenate([carry, carry], axis=1)
        slot = jnp.sum(jnp.where(hit, prior, 0.0), axis=0, keepdims=True).astype(I32)
        carry = carry + counts[:, wide:]
        place = jnp.where(ok, target * AREA + slot, FLAT)
        place_ref[2 * step : 2 * step + 1, :] = place[:, :BLOCK]
        place_ref[2 * step + 1 : 2 * step + 2, :] = place[:, BLOCK:]
        mine = slot_ids == slot
        values = [
            jnp.where(mine, part.astype(F32), 0.0).astype(BF)
            for part in (keys >> 8, keys & 255, *group_code(groups))
        ]
        names_ref[:, at] = names
        values_ref[:, at] = jnp.concatenate(values, axis=0)
        done = (step + 1) * 2
        if done % (blocks // 2) == 0:
            part = pl.ds(done - blocks // 2, blocks // 2)
            places.append(
                pltpu.make_async_copy(
                    place_ref.at[part], place_smem.at[part], sems.at[len(loads) + len(places)]
                )
            )
            places[-1].start()
    packed = lax.dot_general(names_ref[...], values_ref[...], NT, preferred_element_type=F32)
    for d in range(DESTS):
        area_ref[d * AREA + SLOTS : d * AREA + SLOTS + 1, :] = packed[d : d + 1, :BLOCK]
        area_ref[d * AREA + SLOTS + 1 : d * AREA + SLOTS + 2, :] = packed[d : d + 1, BLOCK:]
    loads[-1].wait()

    for n, copy in enumerate(places):
        copy.wait()
        for b in range(n * blocks // 2, (n + 1) * blocks // 2):
            for k in range(BLOCK // 16):
                first = b * BLOCK + k * 16
                x = measures_ref[first : first + 16, :].astype(F32)
                for u in range(16):
                    area_ref[pl.ds(place_smem[b, k * 16 + u], 1), :] = x[u : u + 1, :]

    def give(i, _):
        at = pl.ds(pl.multiple_of(i * 64, 64), 64)
        area16_ref[at, :] = area_ref[at, :].astype(BF)
        return 0

    stores = []
    part = FLAT // PIECES
    for n in range(PIECES):
        lax.fori_loop(n * part // 64, (n + 1) * part // 64, give, 0, unroll=3)
        at = pl.ds(n * part, part)
        stores.append(pltpu.make_async_copy(area16_ref.at[at], out_hbm.at[at], sems.at[9 + n]))
        stores[-1].start()
    for store in stores:
        store.wait()


def pack(bounds, lengths, measures, preds, dest, keys, groups):
    rows = measures.shape[0]
    blocks = rows // BLOCK
    return pl.pallas_call(
        pack_kernel,
        out_shape=jax.ShapeDtypeStruct((FLAT, BLOCK), BF),
        in_specs=[HBM] * 7,
        out_specs=HBM,
        scratch_shapes=[
            pltpu.SMEM(bounds.shape, I32),
            pltpu.SMEM(lengths.shape, I32),
            pltpu.VMEM(measures.shape, BF),
            pltpu.VMEM(preds.shape, I32),
            pltpu.VMEM((blocks, BLOCK), I32),
            pltpu.VMEM((blocks, BLOCK), I32),
            pltpu.VMEM((blocks, BLOCK), I32),
            pltpu.VMEM((FLAT + 8, BLOCK), F32),
            pltpu.VMEM((FLAT, BLOCK), BF),
            pltpu.VMEM((DESTS, rows), BF),
            pltpu.VMEM((4 * SLOTS, rows), BF),
            pltpu.VMEM((blocks, BLOCK), I32),
            pltpu.SMEM((blocks, BLOCK), I32),
            pltpu.SemaphoreType.DMA((9 + PIECES,)),
        ],
        compiler_params=pltpu.CompilerParams(vmem_limit_bytes=58 << 20),
        name="pack",
    )(bounds, lengths, measures, preds, dest, keys, groups)


def add_groups(core, group_ref, pair_ref, sums_ref):
    rows_at = lax.broadcasted_iota(I32, (256, BLOCK), 0).astype(F32).astype(BF)
    one = jnp.ones((), BF)
    zero = jnp.zeros((), BF)
    first = (core * 4).astype(F32)
    for k in range(DESTS // 2 // PER):
        lows = []
        for p in range(k * PER, (k + 1) * PER):
            hi = group_ref[0, p : p + 1, :]
            lows.append((jnp.where(hi >= 8.0, hi - 8.0, hi) - first, group_ref[1, p : p + 1, :]))
        block = pair_ref[k * PER * BLOCK : (k + 1) * PER * BLOCK, :]
        for t in range(0, 4, TILES):
            tiles = []
            for u in range(t, t + TILES):
                cols = []
                for hi, lo in lows:
                    v = jnp.where(hi == float(u), lo, -1.0).astype(BF)
                    cols.append(jnp.where(rows_at == jnp.broadcast_to(v, (256, BLOCK)), one, zero))
                tiles.append(jnp.concatenate(cols, axis=1))
            part = jnp.dot(jnp.concatenate(tiles, axis=0), block, preferred_element_type=F32)
            at = pl.ds(t * 256, TILES * 256)
            if k == 0:
                sums_ref[at, :] = part
            else:
                sums_ref[at, :] = sums_ref[at, :] + part


def join_kernel(me_ref, got_ref, table_ref, other_ref, pair_ref, group_ref, sums_ref, turned_ref, aux_ref):
    blocks = DESTS // 2
    for d in range(DESTS):
        pair = got_ref[d * AREA + SLOTS : (d + 1) * AREA, :].astype(F32)
        aux_ref[:, d : d + 1, :] = pair.reshape(2, 1, BLOCK)

    def halves(n):
        a, b = aux_ref[n, :blocks, :], aux_ref[n, blocks:, :]
        return (
            jnp.concatenate([a[:, :SLOTS], b[:, :SLOTS]], axis=1),
            jnp.concatenate([a[:, SLOTS:], b[:, SLOTS:]], axis=1),
        )

    key_hi, key_lo = halves(0)
    grp_hi, grp_lo = halves(1)
    turned_ref[...] = jnp.concatenate([key_hi * 256.0 + key_lo, grp_hi], axis=0).T
    group_ref[0] = grp_hi
    group_ref[1] = grp_lo
    tab = jnp.concatenate([table_ref[:1024, :], table_ref[1024:, :]], axis=1)
    ids = lax.broadcasted_iota(I32, (BLOCK, 256), 1).astype(F32).astype(BF)
    one = jnp.ones((), BF)
    zero = jnp.zeros((), BF)
    for q in range(0, blocks, FETCH):
        picks = []
        uppers = []
        for p in range(q, q + FETCH):
            key = jnp.broadcast_to(turned_ref[:, p : p + 1], (BLOCK, BLOCK))
            upper = key >= 1024.0
            uppers.append(upper)
            key = jnp.where(upper, key - 1024.0, key)
            cols = []
            for t in range(4):
                k = (key - 256.0 * t).astype(BF)
                k = jnp.concatenate([k, k], axis=1)
                cols.append(jnp.where(ids == k, one, zero))
            picks.append(jnp.concatenate(cols, axis=1))
        found = jnp.dot(jnp.concatenate(picks, axis=0), tab, preferred_element_type=F32)
        for p in range(q, q + FETCH):
            mine = found[(p - q) * BLOCK : (p - q + 1) * BLOCK, :]
            row = jnp.where(uppers[p - q], mine[:, BLOCK:], mine[:, :BLOCK])
            low, high_at = p * AREA, (blocks + p) * AREA
            pay = jnp.concatenate(
                [got_ref[low : low + SLOTS, :], got_ref[high_at : high_at + SLOTS, :]], axis=0
            )
            joined = pay.astype(F32) * row
            high = jnp.broadcast_to(turned_ref[:, blocks + p : blocks + p + 1], (BLOCK, BLOCK)) >= 8.0
            none = jnp.zeros_like(joined)
            to = slice(p * BLOCK, (p + 1) * BLOCK)
            pair_ref[to, :BLOCK] = jnp.where(high, none, joined).astype(BF)
            pair_ref[to, BLOCK:] = jnp.where(high, joined, none).astype(BF)
    add_groups(1 - me_ref[0], group_ref, pair_ref, sums_ref)
    for q in range(64):
        at = slice(q % 32 * 32, (q % 32 + 1) * 32)
        other_ref[q] = sums_ref[at, q // 32 * BLOCK : (q // 32 + 1) * BLOCK].astype(BF)


def join(me, got, table):
    blocks = DESTS // 2
    return pl.pallas_call(
        join_kernel,
        out_shape=(
            jax.ShapeDtypeStruct((64, 32, BLOCK), BF),
            jax.ShapeDtypeStruct((blocks * BLOCK, 2 * BLOCK), BF),
            jax.ShapeDtypeStruct((2, blocks, BLOCK), F32),
        ),
        in_specs=[SMEM, VMEM, VMEM],
        out_specs=(VMEM, VMEM, VMEM),
        scratch_shapes=[
            pltpu.VMEM((1024, 2 * BLOCK), F32),
            pltpu.VMEM((BLOCK, BLOCK), F32),
            pltpu.VMEM((2, DESTS, BLOCK), F32),
        ],
        cost_estimate=pl.CostEstimate(flops=9 << 30, bytes_accessed=8 << 20, transcendentals=0),
        compiler_params=pltpu.CompilerParams(vmem_limit_bytes=30 << 20),
        name="join",
    )(me, got, table)


def rest_kernel(me_ref, pair_ref, group_ref, own_ref, sums_ref):
    add_groups(me_ref[0], group_ref, pair_ref, sums_ref)
    for q in range(64):
        at = slice(q % 32 * 32, (q % 32 + 1) * 32)
        own_ref[q] = sums_ref[at, q // 32 * BLOCK : (q // 32 + 1) * BLOCK]


def rest(me, pair, group):
    return pl.pallas_call(
        rest_kernel,
        out_shape=jax.ShapeDtypeStruct((64, 32, BLOCK), F32),
        in_specs=[SMEM, VMEM, VMEM],
        out_specs=VMEM,
        scratch_shapes=[pltpu.VMEM((1024, 2 * BLOCK), F32)],
        cost_estimate=pl.CostEstimate(flops=5 << 30, bytes_accessed=8 << 20, transcendentals=0),
        compiler_params=pltpu.CompilerParams(vmem_limit_bytes=24 << 20),
        name="rest",
    )(me, pair, group)


def merge_kernel(own_ref, got_ref, out_ref):
    chips, rows, _ = own_ref.shape
    total = (own_ref[...] + got_ref[...].astype(F32)).astype(BF)
    out_ref[:, :rows, :] = total
    ones = jnp.ones((8, BLOCK), BF)
    flat = total.reshape(chips * rows, BLOCK)
    means = lax.dot_general(ones, flat, NT, preferred_element_type=F32)
    score = jnp.concatenate(
        [means[0:1, n * BLOCK : (n + 1) * BLOCK] for n in range(chips * rows // BLOCK)], axis=0
    )
    score = (score * (1.0 / BLOCK)).astype(BF)
    out_ref[:, rows:, :] = jnp.broadcast_to(score[None], (chips, *score.shape))


def merge(own, got):
    chips, rows, _ = own.shape
    return pl.pallas_call(
        merge_kernel,
        out_shape=jax.ShapeDtypeStruct((chips, rows + chips * rows // BLOCK, BLOCK), BF),
        in_specs=[VMEM, VMEM],
        out_specs=VMEM,
        compiler_params=pltpu.CompilerParams(vmem_limit_bytes=16 << 20),
        name="merge",
    )(own, got)


def total_kernel(got_ref, sums_ref, score_ref):
    rows = sums_ref.shape[0]
    total = got_ref[0].astype(F32)
    for p in range(1, got_ref.shape[0]):
        total = total + got_ref[p].astype(F32)
    sums_ref[...] = total[:rows, :]
    score_ref[...] = total[rows:, :]


def total(got, rows):
    return pl.pallas_call(
        total_kernel,
        out_shape=(
            jax.ShapeDtypeStruct((rows, BLOCK), F32),
            jax.ShapeDtypeStruct((got.shape[1] - rows, BLOCK), F32),
        ),
        in_specs=[VMEM],
        out_specs=(VMEM, VMEM),
        compiler_params=pltpu.CompilerParams(vmem_limit_bytes=8 << 20),
        name="total",
    )(got)


def leaders_kernel(sums_ref, a_ref, b_ref, sums_hbm, out_ref, sem):
    copy = pltpu.make_async_copy(sums_ref, sums_hbm, sem)
    copy.start()
    x = jnp.concatenate([a_ref[...], b_ref[...]], axis=0)
    lanes = 4 * BLOCK

    def ids(shape, dim):
        return lax.broadcasted_iota(I32, shape, dim)

    def column(v):
        return jnp.broadcast_to(v, (BLOCK, BLOCK)).T

    best = jnp.max(x, axis=0, keepdims=True)
    down = column(best)
    square = (BLOCK, BLOCK)
    over = (down > best) | ((down == best) & (ids(square, 0) < ids(square, 1)))
    rank = jnp.sum(over.astype(F32), axis=0, keepdims=True).astype(I32)
    pick = (ids((TOPK, BLOCK), 0) == rank).astype(F32)
    copies = jnp.concatenate([x] * TOPK, axis=0)
    tiled = lax.dot_general(
        pick, copies, NT, precision=lax.Precision.HIGHEST, preferred_element_type=F32
    )
    keep = ids((TOPK, lanes), 0) == ids((TOPK, lanes), 1) // x.shape[0]
    flat = jnp.sum(jnp.where(keep, tiled, 0.0), axis=0, keepdims=True)
    pieces = [flat[:, n * BLOCK : (n + 1) * BLOCK] for n in range(4)]
    out = jnp.zeros((1, BLOCK), F32)
    for m in range(4):
        down = column(pieces[m])
        wins = jnp.zeros(square, F32)
        for n in range(4):
            over = pieces[n] > down
            if n < m:
                over = over | (pieces[n] == down)
            elif n == m:
                over = over | ((pieces[n] == down) & (ids(square, 1) < ids(square, 0)))
            wins = wins + over.astype(F32)
        place = jnp.sum(wins, axis=1, keepdims=True).astype(I32)
        out = out + jnp.sum(jnp.where(place == ids(square, 1), down, 0.0), axis=0, keepdims=True)
    out_ref[...] = out[:, :TOPK]
    copy.wait()


def leaders(sums, a, b):
    return pl.pallas_call(
        leaders_kernel,
        out_shape=(
            jax.ShapeDtypeStruct(sums.shape, F32),
            jax.ShapeDtypeStruct((1, TOPK), F32),
        ),
        in_specs=[VMEM, VMEM, VMEM],
        out_specs=(HBM, VMEM),
        scratch_shapes=[pltpu.SemaphoreType.DMA],
        compiler_params=pltpu.CompilerParams(vmem_limit_bytes=4 << 20),
        name="leaders",
    )(sums, a, b)


CHIPS = ("section", "dom_0", "dom_1")
CORE = "dom_2"
DEVICES = (*CHIPS, CORE)
SWAP = [(0, 1), (1, 0)]


def on_device(
    measures, pred_columns, bounds, lengths, destination, key_offset, group_ids, build_table
):
    blocks = measures.shape[0] // BLOCK
    me = lax.axis_index(CORE).astype(I32).reshape(1)

    def lanes(v):
        return v.reshape(blocks, BLOCK)

    me, bounds = lax.optimization_barrier((me, bounds))
    packets = pack(
        bounds, lengths, measures, pred_columns, lanes(destination), lanes(key_offset), lanes(group_ids)
    )
    got = lax.all_to_all(
        packets.reshape(DESTS, AREA // 2, 2, BLOCK), DEVICES, split_axis=0, concat_axis=0, tiled=True
    ).reshape(FLAT, BLOCK)
    theirs, joined, codes = join(me, got, build_table)
    from_partner = lax.ppermute(theirs, CORE, SWAP)
    pair = merge(rest(me, joined, codes), from_partner)
    arrived = lax.all_to_all(pair, CHIPS, split_axis=0, concat_axis=0, tiled=True)
    group_sums, scores = total(arrived, 32)
    group_sums, top = leaders(group_sums, scores, lax.ppermute(scores, CORE, SWAP))
    return group_sums, top.reshape(TOPK)


def solution(mesh):
    finer = Mesh(mesh.devices.reshape(mesh.shape["section"], 4, 4, 2), DEVICES)
    return jax.shard_map(
        on_device,
        mesh=finer,
        in_specs=(
            P(DEVICES, None),
            P(None, DEVICES),
            P(),
            P(DEVICES),
            P(DEVICES, None),
            P(DEVICES),
            P(DEVICES),
            P(DEVICES, None),
        ),
        out_specs=(P(DEVICES, None), P()),
        check_vma=False,
    )
```
